8 devices in a mesh: dp: 1 (over z), tp: 2 (over y), sp: 4 (over x, core).
Axes of the slice: x: 2, y: 2, z: 1, core: 2. Of those that a mesh axis runs over, the one named last changes fastest.
Arguments:
- x_in: bfloat16 [4096, 768], P(('dp', 'sp'))
- w_z: bfloat16 [768, 1536], P(None, 'tp')
- w_x: bfloat16 [768, 1536], P(None, 'tp')
- w_bc: bfloat16 [768, 256], replicated
- w_dt: bfloat16 [768, 24], P(None, 'tp')
- a_neg: float32 [24], P('tp')
- dt_bias: float32 [24], P('tp')
- d_skip: float32 [24], P('tp')
- w_out: bfloat16 [1536, 768], P('tp')
Outputs:
- output: bfloat16 [4096, 768], P(('dp', 'sp', 'tp'))
All inputs are finite; a program needn't handle non-finite values.
Results may differ from the reference program's by a relative error of at most 0.0111934.
Values are sent between devices in bfloat16 or wider.
A program may use at most 1 GiB of HBM per device.

```python
import jax
import jax.numpy as jnp
from jax import lax

D_MODEL = 768
N_HEADS = 24
HEAD_DIM = 64
D_STATE = 128
TOKENS_DEV = 1024
SEQ_DEVS = 4
PIECE_LEN = 64
D_INNER = N_HEADS * HEAD_DIM
SEQ_LEN = SEQ_DEVS * TOKENS_DEV


def setup_inputs(seed: int = 0, part: int = 0) -> dict:
    keys = jax.random.split(jax.random.key(seed), 9)
    x_key = jax.random.fold_in(keys[0], part)
    x_in = jax.random.normal(x_key, (SEQ_LEN, D_MODEL), jnp.float32)
    w_z = jax.random.normal(keys[1], (D_MODEL, D_INNER), jnp.float32) * D_MODEL ** -0.5
    w_x = jax.random.normal(keys[2], (D_MODEL, D_INNER), jnp.float32) * D_MODEL ** -0.5
    bc_scale = D_MODEL ** -0.5 * (D_STATE * TOKENS_DEV) ** -0.25
    w_bc = jax.random.normal(keys[3], (D_MODEL, 2 * D_STATE), jnp.float32) * bc_scale
    w_dt = jax.random.normal(keys[4], (D_MODEL, N_HEADS), jnp.float32) * (0.5 * D_MODEL ** -0.5)
    a_neg = -jax.random.uniform(keys[5], (N_HEADS,), jnp.float32, minval=0.4, maxval=1.6) / TOKENS_DEV
    dt_bias = jax.random.uniform(keys[6], (N_HEADS,), jnp.float32, minval=-1.0, maxval=1.0)
    d_skip = jax.random.uniform(keys[7], (N_HEADS,), jnp.float32, minval=0.5, maxval=1.5)
    w_out = jax.random.normal(keys[8], (D_INNER, D_MODEL), jnp.float32) * D_INNER ** -0.5
    return dict(x_in=x_in.astype(jnp.bfloat16), w_z=w_z.astype(jnp.bfloat16), w_x=w_x.astype(jnp.bfloat16), w_bc=w_bc.astype(jnp.bfloat16), w_dt=w_dt.astype(jnp.bfloat16), a_neg=a_neg, dt_bias=dt_bias, d_skip=d_skip, w_out=w_out.astype(jnp.bfloat16))


def ssd_scan(x_heads, dt_step, log_a, b_mat, c_mat):
    n_pieces = SEQ_LEN // PIECE_LEN
    pieces = (x_heads.reshape(n_pieces, PIECE_LEN, N_HEADS, HEAD_DIM), dt_step.reshape(n_pieces, PIECE_LEN, N_HEADS), log_a.reshape(n_pieces, PIECE_LEN, N_HEADS), b_mat.reshape(n_pieces, PIECE_LEN, D_STATE), c_mat.reshape(n_pieces, PIECE_LEN, D_STATE))
    positions = jnp.arange(PIECE_LEN)
    causal = (positions[:, None] >= positions[None, :])[:, :, None]

    def piece_step(state, piece):
        x_piece, dt_piece, la_piece, b_piece, c_piece = piece
        cum_log = jnp.cumsum(la_piece, axis=0)
        decay = jnp.where(causal, jnp.exp(jnp.minimum(cum_log[:, None, :] - cum_log[None, :, :], 0.0)), 0.0)
        gram = jnp.einsum('tn,sn->ts', c_piece, b_piece)
        weights = gram[:, :, None] * decay * dt_piece[None, :, :]
        y_piece = jnp.einsum('tsh,shp->thp', weights, x_piece)
        y_piece = y_piece + jnp.exp(cum_log)[:, :, None] * jnp.einsum('hpn,tn->thp', state, c_piece)
        to_end = jnp.exp(cum_log[-1][None, :] - cum_log) * dt_piece
        new_state = jnp.exp(cum_log[-1])[:, None, None] * state + jnp.einsum('sh,shp,sn->hpn', to_end, x_piece, b_piece)
        return new_state, y_piece

    init = jnp.zeros((N_HEADS, HEAD_DIM, D_STATE), jnp.float32)
    _, y_all = lax.scan(piece_step, init, pieces)
    return y_all.reshape(SEQ_LEN, N_HEADS, HEAD_DIM)


def reference(x_in, w_z, w_x, w_bc, w_dt, a_neg, dt_bias, d_skip, w_out):
    z_gate = jnp.dot(x_in, w_z, preferred_element_type=jnp.float32).astype(jnp.bfloat16)
    x_proj = jnp.dot(x_in, w_x, preferred_element_type=jnp.float32).astype(jnp.bfloat16)
    bc_val = jnp.dot(x_in, w_bc, preferred_element_type=jnp.float32).astype(jnp.bfloat16).astype(jnp.float32)
    dt_step = jax.nn.softplus(jnp.dot(x_in, w_dt, preferred_element_type=jnp.float32) + dt_bias)
    log_a = dt_step * a_neg
    x_heads = x_proj.astype(jnp.float32).reshape(SEQ_LEN, N_HEADS, HEAD_DIM)
    b_mat = bc_val[:, :D_STATE]
    c_mat = bc_val[:, D_STATE:]
    y_fwd = ssd_scan(x_heads, dt_step, log_a, b_mat, c_mat)
    y_bwd = ssd_scan(x_heads[::-1], dt_step[::-1], log_a[::-1], b_mat[::-1], c_mat[::-1])[::-1]
    y_sum = y_fwd + y_bwd + 2.0 * d_skip[:, None] * x_heads
    gated = (y_sum.reshape(SEQ_LEN, D_INNER) * jax.nn.silu(z_gate.astype(jnp.float32))).astype(jnp.bfloat16)
    mixed = jnp.dot(gated, w_out, preferred_element_type=jnp.float32)
    return (x_in.astype(jnp.float32) + mixed).astype(jnp.bfloat16)
```

```python
import jax
import jax.numpy as jnp
from jax import lax
from jax.experimental import pallas as pl
from jax.experimental.pallas import tpu as pltpu
from jax.sharding import PartitionSpec as P

MESH = pl.DeviceIdType.MESH
F32 = jnp.float32
BF16 = jnp.bfloat16
LOG2E = 1.4426950408889634

CHUNK = 128
LANES = 128
GROUP_COLS = 256


def dot(a, b):
    return jnp.dot(a, b, preferred_element_type=F32)


def split3(v):
    hi = v.astype(BF16)
    rest = v - hi.astype(F32)
    mid = rest.astype(BF16)
    return hi, mid, (rest - mid.astype(F32)).astype(BF16)


def softplus(v):
    return jnp.maximum(v, 0.0) + jnp.log1p(jnp.exp(-jnp.abs(v)))


def kernel(dims, x_hbm, wz_hbm, wx_hbm, wbc_hbm, wdt_hbm, wo_hbm, a_s, bias_s, dskip_s, out_ref,
           x_v, wz_v, wx_v, wbc_v, wdt_v, wo_own, wo_peer, c_v, bt_v, rpad_v, dt_v, ct_v, et_v, cola_v, colb_v, colc_v,
           elo_v, ehi_v, tab_v, gram_v, u_v, z_v, y_v, pf_v, pb_v, hf_v, hb_v, s1_send, s1_recv, dec_send, dec_recv,
           s2_send, s2_recv, g_v, g_recv, acc_v,
           in_sem, s1_ss, s1_rs, dec_ss, dec_rs, s2_ss, s2_rs, wy_ss, wy_rs, wf_ss, wf_rs, g_ss, g_rs):
    tokens, n_head, n_sp = dims
    d_model = x_v.shape[1]
    inner = wx_v.shape[1]
    n_chunk = tokens // CHUNK
    n_half = n_chunk // 2
    half = tokens // 2
    n_grp = inner // GROUP_COLS
    head_dim = inner // n_head
    grp_heads = GROUP_COLS // head_dim
    wrows = inner // n_sp

    tp = lax.axis_index('tp')
    sp = lax.axis_index('sp')
    core = lax.rem(sp, 2)
    partner = sp + 1 - 2 * core
    other_tp = 1 - tp
    my_base = tp * n_half
    peer_base = other_tp * n_half

    def load(src, dst, i):
        return pltpu.make_async_copy(src, dst, in_sem.at[i])

    ld_bc = load(wbc_hbm, wbc_v, 0)
    ld_dt = load(wdt_hbm, wdt_v, 1)
    ld_x = [load(x_hbm.at[pl.ds(i * half, half)], x_v.at[pl.ds(i * half, half)], 2 + i) for i in range(2)]
    ld_wx = load(wx_hbm, wx_v, 4)
    ld_wz = load(wz_hbm, wz_v, 5)
    ld_wo = load(wo_hbm, wo_own, 6)
    for ld in (ld_bc, ld_dt, ld_x[0], ld_x[1], ld_wx, ld_wz):
        ld.start()

    barrier = pltpu.get_barrier_semaphore()
    for step in range(1, n_sp):
        pl.semaphore_signal(barrier, inc=1, device_id={'sp': lax.rem(sp + step, n_sp)}, device_id_type=MESH)
    pl.semaphore_signal(barrier, inc=1, device_id={'tp': other_tp}, device_id_type=MESH)

    row_h = lax.broadcasted_iota(jnp.int32, (16, LANES), 0)
    bias_t = jnp.zeros((16, LANES), F32)
    a_t = jnp.zeros((16, LANES), F32)
    for h in range(n_head):
        bias_t = jnp.where(row_h == h, bias_s[h], bias_t)
        a_t = jnp.where(row_h == h, a_s[h] * LOG2E, a_t)
    sq_r = lax.broadcasted_iota(jnp.int32, (CHUNK, LANES), 0)
    sq_c = lax.broadcasted_iota(jnp.int32, (CHUNK, LANES), 1)
    tri = jnp.concatenate([jnp.where(sq_r <= sq_c, 1.0, 0.0), jnp.where(sq_r < sq_c, 1.0, 0.0)], axis=1).astype(BF16)
    diag2 = jnp.where(sq_r == sq_c, 2.0, 1.0)
    ex_r = lax.broadcasted_iota(jnp.int32, (LANES, inner), 0)
    ex_h = lax.broadcasted_iota(jnp.int32, (LANES, inner), 1) // head_dim
    ex_q = jnp.where(lax.rem(ex_r, 16) == ex_h, 1.0, 0.0)
    elo_v[...] = jnp.where(ex_r < 48, ex_q, 0.0).astype(BF16)
    ehi_v[...] = jnp.where((ex_r >= 64) & (ex_r < 112), ex_q, 0.0).astype(BF16)
    e_one = jnp.where(ex_r[:32] == ex_h[:32], 1.0, 0.0).astype(BF16)
    rpad_v[...] = jnp.zeros_like(rpad_v)

    pl.semaphore_wait(barrier, n_sp)

    my_rows = pl.ds(sp * wrows, wrows)
    wy = pltpu.make_async_remote_copy(src_ref=wo_hbm.at[my_rows], dst_ref=wo_peer.at[my_rows], send_sem=wy_ss, recv_sem=wy_rs,
                                      device_id={'tp': other_tp}, device_id_type=MESH)
    wy.start()

    ld_bc.wait()
    ld_dt.wait()
    for i in range(2):
        ld_x[i].wait()
        rows = slice(i * half, (i + 1) * half)
        x_half = x_v[rows, :]
        bc_val = dot(x_half, wbc_v[...]).astype(BF16)
        c_v[rows, :] = bc_val[:, LANES:]
        rpad_v[rows, 0:n_head] = lax.dot_general(x_half, wdt_v[...], (((1,), (1,)), ((), ())), preferred_element_type=F32)
        for k in range(n_half):
            c = i * n_half + k
            bt_v[c] = bc_val[k * CHUNK:(k + 1) * CHUNK, :LANES].astype(F32).T.astype(BF16)
            dt_v[c] = softplus(rpad_v[c * CHUNK:(c + 1) * CHUNK, :].T[:16] + bias_t)
    ld_wo.start()

    dt_all = dt_v[...].reshape(n_chunk * 16, LANES)
    la_all = (dt_v[...] * a_t[None]).reshape(n_chunk * 16, LANES)
    cum = sum(dot(part, tri) for part in split3(la_all))
    c_log = cum[:, :LANES]
    e_log = cum[:, LANES:]
    ct_v[...] = c_log.reshape(n_chunk, 16, LANES)
    et_v[...] = e_log.reshape(n_chunk, 16, LANES)
    tail = c_log[:, LANES - 1:LANES]
    parts_ef = split3(jnp.exp2(c_log))
    parts_eb = split3(jnp.exp2(tail - e_log))
    parts_wf = split3(jnp.exp2(tail - c_log) * dt_all)
    parts_wb = split3(jnp.exp2(e_log) * dt_all)
    blank = jnp.zeros((16, LANES), F32)

    def column_tile(first, second, c):
        rows = slice(c * 16, (c + 1) * 16)
        tile = [p[rows].astype(F32) for p in first] + [blank] + [p[rows].astype(F32) for p in second] + [blank]
        return jnp.concatenate(tile, axis=0).T.astype(BF16)

    run = jnp.zeros((1, 32), F32)
    tails, starts, ends = [], [], []
    for c in range(n_chunk):
        rows = slice(c * 16, (c + 1) * 16)
        colb_v[c] = column_tile(parts_wf, parts_wb, c)
        col = jnp.concatenate([c_log[rows], e_log[rows]], axis=0).T
        colc_v[c] = col
        last = col[CHUNK - 1:CHUNK, :]
        tails.append(last)
        starts.append(run)
        run = run + last
        ends.append(run)
    logs = jnp.concatenate(tails + starts + [run - e for e in ends] + [run] * n_chunk, axis=0)
    tab = sum(dot(part, e_one) for part in split3(jnp.exp2(logs)))
    for i in range(3 * n_chunk + 1):
        tab_v[i] = tab[i:i + 1, :]
    dec_send[...] = tab[3 * n_chunk:, :]
    for c in range(n_chunk):
        cola_v[c] = column_tile(parts_ef, parts_eb, c)

    def to_partner(g):
        return pltpu.make_async_remote_copy(src_ref=s1_send.at[g], dst_ref=s1_recv.at[g], send_sem=s1_ss.at[g], recv_sem=s1_rs.at[g],
                                            device_id={'sp': partner}, device_id_type=MESH)

    def to_chip(g, t):
        return pltpu.make_async_remote_copy(src_ref=s2_send.at[g], dst_ref=s2_recv.at[g], send_sem=s2_ss.at[g, t], recv_sem=s2_rs.at[g],
                                            device_id={'sp': 2 - 2 * (sp // 2) + t}, device_id_type=MESH)

    def to_peer(g, k):
        return pltpu.make_async_remote_copy(src_ref=g_v.at[g, peer_base + k], dst_ref=g_recv.at[g, k], send_sem=g_ss.at[g, k],
                                            recv_sem=g_rs.at[g, k], device_id={'tp': other_tp}, device_id_type=MESH)

    def gather(step):
        return pltpu.make_async_remote_copy(src_ref=wo_peer.at[my_rows], dst_ref=wo_peer.at[my_rows], send_sem=wf_ss.at[step - 1],
                                            recv_sem=wf_rs.at[step - 1], device_id={'sp': lax.rem(sp + step, n_sp)}, device_id_type=MESH)

    dec_copy = pltpu.make_async_remote_copy(src_ref=dec_send, dst_ref=dec_recv, send_sem=dec_ss, recv_sem=dec_rs,
                                            device_id={'sp': partner}, device_id_type=MESH)
    dec_copy.start()

    def states(g):
        cols = slice(g * GROUP_COLS, (g + 1) * GROUP_COLS)
        for i in range(2):
            rows = slice(i * half, (i + 1) * half)
            u_v[g, rows, :] = dot(x_v[rows, :], wx_v[:, cols]).astype(BF16)
        elo = elo_v[:, cols]
        ehi = ehi_v[:, cols]
        st_f, st_b = [], []
        for c in range(n_chunk):
            u_c = u_v[g, c * CHUNK:(c + 1) * CHUNK, :].astype(F32)
            st_f.append(dot(bt_v[c], (u_c * dot(colb_v[c], elo)).astype(BF16)))
            st_b.append(dot(bt_v[c], (u_c * dot(colb_v[c], ehi)).astype(BF16)))
        acc = jnp.zeros((LANES, GROUP_COLS), F32)
        for c in range(n_chunk):
            pf_v[g, c] = acc
            acc = tab_v[c][:, cols] * acc + st_f[c]
        pf_v[g, n_chunk] = acc
        acc = jnp.zeros((LANES, GROUP_COLS), F32)
        for c in reversed(range(n_chunk)):
            pb_v[g, c] = acc
            acc = tab_v[c][:, cols] * acc + st_b[c]
        pb_v[g, n_chunk] = acc
        s1_send[g] = jnp.where(core == 0, pf_v[g, n_chunk], acc).astype(BF16)
        to_partner(g).start()

    sends_far = (sp == 1) | (sp == 2)

    def pass_on(g):
        to_partner(g).wait_recv()

        @pl.when(sends_far)
        def _():
            cols = slice(g * GROUP_COLS, (g + 1) * GROUP_COLS)
            own = jnp.where(core == 1, pf_v[g, n_chunk], pb_v[g, n_chunk])
            s2_send[g] = (own + tab_v[3 * n_chunk][:, cols] * s1_recv[g].astype(F32)).astype(BF16)
            to_chip(g, 0).start()
            to_chip(g, 1).start()

    def incoming(g):
        to_chip(g, 0).wait_recv()
        cols = slice(g * GROUP_COLS, (g + 1) * GROUP_COLS)
        near = s1_recv[g].astype(F32)
        far = s2_recv[g].astype(F32)
        both = near + dec_recv[0:1, cols] * far
        hf_v[g] = jnp.where(sp == 0, 0.0, jnp.where(sp == 1, near, jnp.where(sp == 2, far, both)))
        hb_v[g] = jnp.where(sp == 3, 0.0, jnp.where(sp == 2, near, jnp.where(sp == 1, far, both)))

    lane = lax.broadcasted_iota(jnp.int32, (CHUNK, LANES), 1)
    low_lane = lane < head_dim

    def z_part(g, base):
        cols = slice(g * GROUP_COLS, (g + 1) * GROUP_COLS)
        rows = pl.ds(pl.multiple_of(base * CHUNK, CHUNK), half)
        z_v[g, rows, :] = dot(x_v[rows, :], wz_v[:, cols]).astype(BF16)

    def intra(g, c):
        rows = pl.ds(pl.multiple_of(c * CHUNK, CHUNK), CHUNK)
        gram = gram_v[c]
        for p in range(grp_heads // 2):
            lanes = slice(p * LANES, (p + 1) * LANES)
            u_pair = u_v[g, rows, lanes]
            weights = []
            for h in (g * grp_heads + 2 * p, g * grp_heads + 2 * p + 1):
                arg = jnp.minimum(colc_v[c, :, h:h + 1] - ct_v[c, h:h + 1, :], et_v[c, h:h + 1, :] - colc_v[c, :, 16 + h:17 + h])
                weights.append((gram * jnp.exp2(arg) * dt_v[c, h:h + 1, :]).astype(BF16))
            zero = jnp.zeros_like(u_pair)
            u_diag = jnp.concatenate([jnp.where(low_lane, u_pair, zero), jnp.where(low_lane, zero, u_pair)], axis=0)
            h0 = g * grp_heads + 2 * p
            skip = jnp.where(low_lane[:1], 2.0 * dskip_s[h0], 2.0 * dskip_s[h0 + 1])
            y_v[g, rows, lanes] = dot(jnp.concatenate(weights, axis=1), u_diag) + skip * u_pair.astype(F32)

    def finish(g, c):
        cols = slice(g * GROUP_COLS, (g + 1) * GROUP_COLS)
        rows = pl.ds(pl.multiple_of(c * CHUNK, CHUNK), CHUNK)
        in_f = (pf_v[g, c] + tab_v[n_chunk + c][:, cols] * hf_v[g]).astype(BF16)
        in_b = (pb_v[g, c] + tab_v[2 * n_chunk + c][:, cols] * hb_v[g]).astype(BF16)
        c_mat = c_v[rows, :]
        y = y_v[g, rows, :] + dot(cola_v[c], elo_v[:, cols]) * dot(c_mat, in_f) + dot(cola_v[c], ehi_v[:, cols]) * dot(c_mat, in_b)
        hz = 0.5 * z_v[g, rows, :].astype(F32)
        g_v[g, c] = (y * (hz + hz * jnp.tanh(hz))).astype(BF16)

    ld_wx.wait()
    states(0)
    for c in range(n_chunk):
        gram_v[c] = dot(c_v[c * CHUNK:(c + 1) * CHUNK, :], bt_v[c]) * diag2
    states(1)
    pass_on(0)
    states(2)
    pass_on(1)
    ld_wz.wait()
    z_part(0, peer_base)
    for k in range(n_half):
        intra(0, peer_base + k)
    pass_on(2)
    dec_copy.wait_recv()
    for g in range(n_grp):
        if g > 0:
            z_part(g, peer_base)
            for k in range(n_half):
                intra(g, peer_base + k)
        incoming(g)
        for k in range(n_half):
            finish(g, peer_base + k)
            to_peer(g, k).start()
        if g == 0:
            wy.wait_recv()
            for step in range(1, n_sp):
                gather(step).start()

    for g in range(n_grp):
        z_part(g, my_base)
        for k in range(n_half):
            intra(g, my_base + k)
        for k in range(n_half):
            finish(g, my_base + k)
    ld_wo.wait()
    my_tokens = pl.ds(pl.multiple_of(my_base * CHUNK, CHUNK), half)
    acc_v[...] = x_v[my_tokens, :].astype(F32)
    for g in range(n_grp):
        mine = g_v[g, pl.ds(my_base, n_half)].reshape(half, GROUP_COLS)
        acc_v[...] += dot(mine, wo_own[g * GROUP_COLS:(g + 1) * GROUP_COLS, :])
    for step in range(1, n_sp):
        gather(step).wait_recv()
    for g in range(n_grp):
        w_g = wo_peer[g * GROUP_COLS:(g + 1) * GROUP_COLS, :]
        for k in range(n_half):
            to_peer(g, k).wait_recv()
            rows = slice(k * CHUNK, (k + 1) * CHUNK)
            val = acc_v[rows, :] + dot(g_recv[g, k], w_g)
            if g < n_grp - 1:
                acc_v[rows, :] = val
            else:
                out_ref[rows, :] = val.astype(BF16)

    wy.wait_send()
    dec_copy.wait_send()
    for step in range(1, n_sp):
        gather(step).wait_send()
    for g in range(n_grp):
        to_partner(g).wait_send()

        @pl.when(sends_far)
        def _():
            to_chip(g, 0).wait_send()
            to_chip(g, 1).wait_send()
        for k in range(n_half):
            to_peer(g, k).wait_send()


def solution(mesh):
    n_sp = mesh.shape['sp']

    def device_fn(x_blk, w_z, w_x, w_bc, w_dt, a_neg, dt_bias, d_skip, w_out):
        tokens, d_model = x_blk.shape
        n_head = a_neg.shape[0]
        inner = w_x.shape[1]
        half = tokens // 2
        n_chunk = tokens // CHUNK
        n_half = n_chunk // 2
        n_grp = inner // GROUP_COLS
        vmem = pltpu.VMEM
        dma = pltpu.SemaphoreType.DMA
        state = (n_grp, LANES, GROUP_COLS)
        hbm = pl.BlockSpec(memory_space=pl.ANY)
        smem = pl.BlockSpec(memory_space=pltpu.SMEM)

        def body(*refs):
            kernel((tokens, n_head, n_sp), *refs)

        return pl.pallas_call(
            body,
            out_shape=jax.ShapeDtypeStruct((half, d_model), BF16),
            in_specs=[hbm] * 6 + [smem] * 3,
            out_specs=pl.BlockSpec(memory_space=pltpu.VMEM),
            scratch_shapes=[
                vmem((tokens, d_model), BF16), vmem((d_model, inner), BF16), vmem((d_model, inner), BF16),
                vmem(w_bc.shape, BF16), vmem(w_dt.shape[::-1], BF16), vmem((inner, d_model), BF16), vmem((inner, d_model), BF16),
                vmem((tokens, LANES), BF16), vmem((n_chunk, LANES, CHUNK), BF16), vmem((tokens, LANES), F32),
                vmem((n_chunk, 16, LANES), F32), vmem((n_chunk, 16, LANES), F32), vmem((n_chunk, 16, LANES), F32),
                vmem((n_chunk, CHUNK, LANES), BF16), vmem((n_chunk, CHUNK, LANES), BF16), vmem((n_chunk, CHUNK, 32), F32),
                vmem((LANES, inner), BF16), vmem((LANES, inner), BF16), vmem((3 * n_chunk + 1, 1, inner), F32),
                vmem((n_chunk, CHUNK, CHUNK), F32),
                vmem((n_grp, tokens, GROUP_COLS), BF16), vmem((n_grp, tokens, GROUP_COLS), BF16), vmem((n_grp, tokens, GROUP_COLS), F32),
                vmem((n_grp, n_chunk + 1, LANES, GROUP_COLS), F32), vmem((n_grp, n_chunk + 1, LANES, GROUP_COLS), F32),
                vmem(state, F32), vmem(state, F32), vmem(state, BF16), vmem(state, BF16),
                vmem((8, inner), F32), vmem((8, inner), F32), vmem(state, BF16), vmem(state, BF16),
                vmem((n_grp, n_chunk, CHUNK, GROUP_COLS), BF16), vmem((n_grp, n_half, CHUNK, GROUP_COLS), BF16),
                vmem((half, d_model), F32),
                dma((7,)), dma((n_grp,)), dma((n_grp,)), dma, dma, dma((n_grp, 2)), dma((n_grp,)),
                dma, dma, dma((n_sp - 1,)), dma((n_sp - 1,)), dma((n_grp, n_half)), dma((n_grp, n_half)),
            ],
            compiler_params=pltpu.CompilerParams(collective_id=0, has_side_effects=True),
            cost_estimate=pl.CostEstimate(flops=8 * 10 ** 9, bytes_accessed=8 * 10 ** 6, transcendentals=4 * 10 ** 6),
            name='mamba_layer',
        )(x_blk, w_z, w_x, w_bc, w_dt.T, w_out, a_neg, dt_bias, d_skip)

    in_specs = (P(('dp', 'sp'), None), P(None, 'tp'), P(None, 'tp'), P(None, None), P(None, 'tp'), P('tp'), P('tp'), P('tp'), P('tp', None))
    out_specs = P(('dp', 'sp', 'tp'), None)
    return jax.shard_map(device_fn, mesh=mesh, in_specs=in_specs, out_specs=out_specs, check_vma=False)
```

```python
import jax
import jax.numpy as jnp
from jax import lax
from jax.experimental import pallas as pl
from jax.experimental.pallas import tpu as pltpu
from jax.sharding import PartitionSpec as P

MESH = pl.DeviceIdType.MESH
F32 = jnp.float32
BF16 = jnp.bfloat16
LOG2E = 1.4426950408889634

CHUNK = 128
LANES = 128
GROUPS = (1, 2, 3)


def dot(a, b):
    return jnp.dot(a, b, preferred_element_type=F32)


def split3(v):
    hi = v.astype(BF16)
    rest = v - hi.astype(F32)
    mid = rest.astype(BF16)
    return hi, mid, (rest - mid.astype(F32)).astype(BF16)


def softplus(v):
    return jnp.maximum(v, 0.0) + jnp.log1p(jnp.exp(-jnp.abs(v)))


def kernel(dims, x_hbm, wz_hbm, wx_hbm, wbc_hbm, wdt_hbm, wo_hbm, a_s, bias_s, dskip_s, out_ref,
           x_v, wz_v, wx_v, w0_v, wbc_v, wdt_v, wo_own, wo_peer, c_v, bt_v, wide_v, dt_v, ct_v, et_v, cola_v, colb_v, colc_v,
           elo_v, ehi_v, tab_v, gram_v, u_v, z_v, y_v, pf_v, pb_v, hf_v, hb_v, dec_send, dec_recv, acc_v,
           s1_send, s1_recv, s2_send, s2_recv, g_v, g_recv,
           in_sem, s1_ss, s1_rs, dec_ss, dec_rs, s2_ss, s2_rs, wy_ss, wy_rs, wf_ss, wf_rs, g_ss, g_rs):
    tokens, n_head, n_sp = dims
    d_model = x_v.shape[1]
    inner = wx_v.shape[1]
    n_chunk = tokens // CHUNK
    n_half = n_chunk // 2
    half = tokens // 2
    n_grp = len(GROUPS)
    head_dim = inner // n_head
    edge = [LANES * sum(GROUPS[:g]) for g in range(n_grp + 1)]
    wrows = inner // n_sp

    tp = lax.axis_index('tp')
    sp = lax.axis_index('sp')
    core = lax.rem(sp, 2)
    partner = sp + 1 - 2 * core
    other_tp = 1 - tp
    my_base = tp * n_half
    peer_base = other_tp * n_half

    def load(src, dst, i):
        return pltpu.make_async_copy(src, dst, in_sem.at[i])

    ld_bc = load(wbc_hbm, wbc_v, 0)
    ld_dt = load(wdt_hbm, wdt_v, 1)
    ld_x = [load(x_hbm.at[pl.ds(i * half, half)], x_v.at[pl.ds(i * half, half)], 2 + i) for i in range(2)]
    late = pl.ds(LANES, inner - LANES)
    ld_wx = load(wx_hbm.at[:, late], wx_v.at[:, late], 4)
    ld_w0 = load(wx_hbm.at[:, pl.ds(0, LANES)], w0_v.at[:, pl.ds(0, LANES)], 7)
    ld_wz = load(wz_hbm, wz_v, 5)
    ld_wo = load(wo_hbm, wo_own, 6)
    for ld in (ld_dt, ld_x[0], ld_w0, ld_x[1], ld_bc):
        ld.start()

    barrier = pltpu.get_barrier_semaphore()
    for step in range(1, n_sp):
        pl.semaphore_signal(barrier, inc=1, device_id={'sp': lax.rem(sp + step, n_sp)}, device_id_type=MESH)
    pl.semaphore_signal(barrier, inc=1, device_id={'tp': other_tp}, device_id_type=MESH)

    pl.semaphore_wait(barrier, n_sp)

    my_rows = pl.ds(sp * wrows, wrows)
    wy = pltpu.make_async_remote_copy(src_ref=wo_hbm.at[my_rows], dst_ref=wo_peer.at[my_rows], send_sem=wy_ss, recv_sem=wy_rs,
                                      device_id={'tp': other_tp}, device_id_type=MESH)
    wy.start()
    ld_wx.start()

    row_h = lax.broadcasted_iota(jnp.int32, (16, LANES), 0)
    bias_t = jnp.zeros((16, LANES), F32)
    a_t = jnp.zeros((16, LANES), F32)
    for h in range(n_head):
        bias_t = jnp.where(row_h == h, bias_s[h], bias_t)
        a_t = jnp.where(row_h == h, a_s[h] * LOG2E, a_t)
    sq_r = lax.broadcasted_iota(jnp.int32, (CHUNK, LANES), 0)
    sq_c = lax.broadcasted_iota(jnp.int32, (CHUNK, LANES), 1)
    tri = jnp.concatenate([jnp.where(sq_r <= sq_c, 1.0, 0.0), jnp.where(sq_r < sq_c, 1.0, 0.0)], axis=1).astype(BF16)
    diag2 = jnp.where(sq_r == sq_c, 2.0, 1.0)
    ex_r = lax.broadcasted_iota(jnp.int32, (LANES, inner), 0)
    ex_h = lax.broadcasted_iota(jnp.int32, (LANES, inner), 1) >> (head_dim.bit_length() - 1)
    ex_q = jnp.where((ex_r & 15) == ex_h, 1.0, 0.0)
    elo_v[...] = jnp.where(ex_r < 48, ex_q, 0.0).astype(BF16)
    ehi_v[...] = jnp.where((ex_r >= 64) & (ex_r < 112), ex_q, 0.0).astype(BF16)
    e_one = jnp.where(ex_r[:32] == ex_h[:32], 1.0, 0.0).astype(BF16)
    wide_v[...] = jnp.zeros_like(wide_v)
    ld_dt.wait()
    wide_v[0:n_head, :] = wdt_v[...].astype(F32)
    for k in range(d_model // LANES):
        rows = slice(k * LANES, (k + 1) * LANES)
        w0_v[rows, LANES:] = wide_v[:, rows].T.astype(BF16)

    ld_w0.wait()
    for i in range(2):
        ld_x[i].wait()
        rows = slice(i * half, (i + 1) * half)
        first = dot(x_v[rows, :], w0_v[...])
        u_v[rows, :LANES] = first[:, :LANES].astype(BF16)
        for k in range(n_half):
            dt_v[i * n_half + k] = softplus(first[k * CHUNK:(k + 1) * CHUNK, LANES:].T[:16] + bias_t)
    ld_bc.wait()
    for i in range(2):
        rows = slice(i * half, (i + 1) * half)
        bc_val = dot(x_v[rows, :], wbc_v[...]).astype(BF16)
        c_v[rows, :] = bc_val[:, LANES:]
        for k in range(n_half):
            bt_v[i * n_half + k] = bc_val[k * CHUNK:(k + 1) * CHUNK, :LANES].astype(F32).T.astype(BF16)

    dt_all = dt_v[...].reshape(n_chunk * 16, LANES)
    la_all = (dt_v[...] * a_t[None]).reshape(n_chunk * 16, LANES)
    cum = sum(dot(part, tri) for part in split3(la_all))
    c_log = cum[:, :LANES]
    e_log = cum[:, LANES:]
    ct_v[...] = c_log.reshape(n_chunk, 16, LANES)
    et_v[...] = e_log.reshape(n_chunk, 16, LANES)
    tail = c_log[:, LANES - 1:LANES]
    parts_ef = split3(jnp.exp2(c_log))
    parts_eb = split3(jnp.exp2(tail - e_log))
    parts_wf = split3(jnp.exp2(tail - c_log) * dt_all)
    parts_wb = split3(jnp.exp2(e_log) * dt_all)
    blank = jnp.zeros((16, LANES), F32)

    def column_tile(first, second, c):
        rows = slice(c * 16, (c + 1) * 16)
        tile = [p[rows].astype(F32) for p in first] + [blank] + [p[rows].astype(F32) for p in second] + [blank]
        return jnp.concatenate(tile, axis=0).T.astype(BF16)

    run = jnp.zeros((1, 32), F32)
    tails, starts, ends = [], [], []
    for c in range(n_chunk):
        rows = slice(c * 16, (c + 1) * 16)
        colb_v[c] = column_tile(parts_wf, parts_wb, c)
        col = jnp.concatenate([c_log[rows], e_log[rows]], axis=0).T
        colc_v[c] = col
        last = col[CHUNK - 1:CHUNK, :]
        tails.append(last)
        starts.append(run)
        run = run + last
        ends.append(run)
    logs = jnp.concatenate(tails + starts + [run - e for e in ends] + [run] * n_chunk, axis=0)
    tab = sum(dot(part, e_one) for part in split3(jnp.exp2(logs)))
    for i in range(3 * n_chunk + 1):
        tab_v[i] = tab[i:i + 1, :]
    dec_send[...] = tab[3 * n_chunk:, :]

    ld_wz.start()
    ld_wo.start()

    def to_partner(g):
        return pltpu.make_async_remote_copy(src_ref=s1_send[g], dst_ref=s1_recv[g], send_sem=s1_ss.at[g], recv_sem=s1_rs.at[g],
                                            device_id={'sp': partner}, device_id_type=MESH)

    def to_chip(g, t):
        return pltpu.make_async_remote_copy(src_ref=s2_send[g], dst_ref=s2_recv[g], send_sem=s2_ss.at[g, t], recv_sem=s2_rs.at[g],
                                            device_id={'sp': 2 - 2 * (sp // 2) + t}, device_id_type=MESH)

    def to_peer(g, k):
        return pltpu.make_async_remote_copy(src_ref=g_v[g].at[peer_base + k], dst_ref=g_recv[g].at[k], send_sem=g_ss.at[g, k],
                                            recv_sem=g_rs.at[g, k], device_id={'tp': other_tp}, device_id_type=MESH)

    def gather(step):
        return pltpu.make_async_remote_copy(src_ref=wo_peer.at[my_rows], dst_ref=wo_peer.at[my_rows], send_sem=wf_ss.at[step - 1],
                                            recv_sem=wf_rs.at[step - 1], device_id={'sp': lax.rem(sp + step, n_sp)}, device_id_type=MESH)

    dec_copy = pltpu.make_async_remote_copy(src_ref=dec_send, dst_ref=dec_recv, send_sem=dec_ss, recv_sem=dec_rs,
                                            device_id={'sp': partner}, device_id_type=MESH)
    dec_copy.start()

    def states(g):
        cols = slice(edge[g], edge[g + 1])
        if g > 0:
            for i in range(2):
                rows = slice(i * half, (i + 1) * half)
                u_v[rows, cols] = dot(x_v[rows, :], wx_v[:, cols]).astype(BF16)
        elo = elo_v[:, cols]
        ehi = ehi_v[:, cols]
        st_f, st_b = [], []
        for c in range(n_chunk):
            u_c = u_v[c * CHUNK:(c + 1) * CHUNK, cols].astype(F32)
            st_f.append(dot(bt_v[c], (u_c * dot(colb_v[c], elo)).astype(BF16)))
            st_b.append(dot(bt_v[c], (u_c * dot(colb_v[c], ehi)).astype(BF16)))
        acc = jnp.zeros((LANES, edge[g + 1] - edge[g]), F32)
        for c in range(n_chunk):
            pf_v[c, :, cols] = acc
            acc = tab_v[c][:, cols] * acc + st_f[c]
        pf_v[n_chunk, :, cols] = acc
        acc = jnp.zeros((LANES, edge[g + 1] - edge[g]), F32)
        for c in reversed(range(n_chunk)):
            pb_v[c, :, cols] = acc
            acc = tab_v[c][:, cols] * acc + st_b[c]
        pb_v[n_chunk, :, cols] = acc
        s1_send[g][...] = jnp.where(core == 0, pf_v[n_chunk, :, cols], acc).astype(BF16)
        to_partner(g).start()

    sends_far = (sp == 1) | (sp == 2)

    def pass_on(g):
        to_partner(g).wait_recv()

        @pl.when(sends_far)
        def _():
            cols = slice(edge[g], edge[g + 1])
            own = jnp.where(core == 1, pf_v[n_chunk, :, cols], pb_v[n_chunk, :, cols])
            s2_send[g][...] = (own + tab_v[3 * n_chunk][:, cols] * s1_recv[g][...].astype(F32)).astype(BF16)
            to_chip(g, 0).start()
            to_chip(g, 1).start()

    def incoming(g):
        to_chip(g, 0).wait_recv()
        cols = slice(edge[g], edge[g + 1])
        near = s1_recv[g][...].astype(F32)
        far = s2_recv[g][...].astype(F32)
        both = near + dec_recv[0:1, cols] * far
        hf_v[:, cols] = jnp.where(sp == 0, 0.0, jnp.where(sp == 1, near, jnp.where(sp == 2, far, both)))
        hb_v[:, cols] = jnp.where(sp == 3, 0.0, jnp.where(sp == 2, near, jnp.where(sp == 1, far, both)))

    lane = lax.broadcasted_iota(jnp.int32, (CHUNK, LANES), 1)
    low_lane = lane < head_dim

    def z_part(g, base):
        cols = slice(edge[g], edge[g + 1])
        rows = pl.ds(pl.multiple_of(base * CHUNK, CHUNK), half)
        z_v[rows, cols] = dot(x_v[rows, :], wz_v[:, cols]).astype(BF16)

    def intra(g, c):
        rows = pl.ds(pl.multiple_of(c * CHUNK, CHUNK), CHUNK)
        gram = gram_v[c]
        for lo in range(edge[g], edge[g + 1], LANES):
            lanes = slice(lo, lo + LANES)
            h0 = lo // head_dim
            u_pair = u_v[rows, lanes]
            weights = []
            for h in (h0, h0 + 1):
                arg = jnp.minimum(colc_v[c, :, h:h + 1] - ct_v[c, h:h + 1, :], et_v[c, h:h + 1, :] - colc_v[c, :, 16 + h:17 + h])
                weights.append((gram * jnp.exp2(arg) * dt_v[c, h:h + 1, :]).astype(BF16))
            zero = jnp.zeros_like(u_pair)
            u_diag = jnp.concatenate([jnp.where(low_lane, u_pair, zero), jnp.where(low_lane, zero, u_pair)], axis=0)
            skip = jnp.where(low_lane[:1], 2.0 * dskip_s[h0], 2.0 * dskip_s[h0 + 1])
            y_v[rows, lanes] = dot(jnp.concatenate(weights, axis=1), u_diag) + skip * u_pair.astype(F32)

    def finish(g, c):
        cols = slice(edge[g], edge[g + 1])
        rows = pl.ds(pl.multiple_of(c * CHUNK, CHUNK), CHUNK)
        in_f = (pf_v[c, :, cols] + tab_v[n_chunk + c][:, cols] * hf_v[:, cols]).astype(BF16)
        in_b = (pb_v[c, :, cols] + tab_v[2 * n_chunk + c][:, cols] * hb_v[:, cols]).astype(BF16)
        c_mat = c_v[rows, :]
        y = y_v[rows, cols] + dot(cola_v[c], elo_v[:, cols]) * dot(c_mat, in_f) + dot(cola_v[c], ehi_v[:, cols]) * dot(c_mat, in_b)
        hz = 0.5 * z_v[rows, cols].astype(F32)
        g_v[g][c] = (y * (hz + hz * jnp.tanh(hz))).astype(BF16)

    states(0)
    for c in range(n_chunk):
        gram_v[c] = dot(c_v[c * CHUNK:(c + 1) * CHUNK, :], bt_v[c]) * diag2
        cola_v[c] = column_tile(parts_ef, parts_eb, c)
    ld_wx.wait()
    states(1)
    pass_on(0)
    states(2)
    pass_on(1)
    ld_wz.wait()
    for g in range(n_grp):
        z_part(g, peer_base)
        for k in range(n_half):
            intra(g, peer_base + k)
        if g == 0:
            pass_on(2)
            dec_copy.wait_recv()
        incoming(g)
        for k in range(n_half):
            finish(g, peer_base + k)
            to_peer(g, k).start()
        if g == 0:
            wy.wait_recv()
            for step in range(1, n_sp):
                gather(step).start()

    for g in range(n_grp):
        z_part(g, my_base)
        for k in range(n_half):
            intra(g, my_base + k)
        for k in range(n_half):
            finish(g, my_base + k)
    ld_wo.wait()
    my_tokens = pl.ds(pl.multiple_of(my_base * CHUNK, CHUNK), half)
    acc_v[...] = x_v[my_tokens, :].astype(F32)
    for g in range(n_grp):
        mine = g_v[g][pl.ds(my_base, n_half)].reshape(half, edge[g + 1] - edge[g])
        acc_v[...] += dot(mine, wo_own[edge[g]:edge[g + 1], :])
    for step in range(1, n_sp):
        gather(step).wait_recv()
    for g in range(n_grp):
        w_g = wo_peer[edge[g]:edge[g + 1], :]
        for k in range(n_half):
            to_peer(g, k).wait_recv()
            rows = slice(k * CHUNK, (k + 1) * CHUNK)
            val = acc_v[rows, :] + dot(g_recv[g][k], w_g)
            if g < n_grp - 1:
                acc_v[rows, :] = val
            else:
                out_ref[rows, :] = val.astype(BF16)

    wy.wait_send()
    dec_copy.wait_send()
    for step in range(1, n_sp):
        gather(step).wait_send()
    for g in range(n_grp):
        to_partner(g).wait_send()

        @pl.when(sends_far)
        def _():
            to_chip(g, 0).wait_send()
            to_chip(g, 1).wait_send()
        for k in range(n_half):
            to_peer(g, k).wait_send()


def solution(mesh):
    n_sp = mesh.shape['sp']

    def device_fn(x_blk, w_z, w_x, w_bc, w_dt, a_neg, dt_bias, d_skip, w_out):
        tokens, d_model = x_blk.shape
        n_head = a_neg.shape[0]
        inner = w_x.shape[1]
        half = tokens // 2
        n_chunk = tokens // CHUNK
        n_half = n_chunk // 2
        n_grp = len(GROUPS)
        wide = [LANES * p for p in GROUPS]
        vmem = pltpu.VMEM
        dma = pltpu.SemaphoreType.DMA
        state = [vmem((LANES, w), BF16) for w in wide]
        hbm = pl.BlockSpec(memory_space=pltpu.HBM)
        smem = pl.BlockSpec(memory_space=pltpu.SMEM)

        def body(*refs):
            kernel((tokens, n_head, n_sp), *refs)

        return pl.pallas_call(
            body,
            out_shape=pltpu.VMEM((half, d_model), BF16),
            in_specs=[hbm] * 6 + [smem] * 3,
            out_specs=pl.BlockSpec(memory_space=pltpu.VMEM),
            scratch_shapes=[
                vmem((tokens, d_model), BF16), vmem((d_model, inner), BF16), vmem((d_model, inner), BF16), vmem((d_model, 2 * LANES), BF16),
                vmem(w_bc.shape, BF16), vmem(w_dt.shape[::-1], BF16), vmem((inner, d_model), BF16), vmem((inner, d_model), BF16),
                vmem((tokens, LANES), BF16), vmem((n_chunk, LANES, CHUNK), BF16), vmem((LANES, d_model), F32),
                vmem((n_chunk, 16, LANES), F32), vmem((n_chunk, 16, LANES), F32), vmem((n_chunk, 16, LANES), F32),
                vmem((n_chunk, CHUNK, LANES), BF16), vmem((n_chunk, CHUNK, LANES), BF16), vmem((n_chunk, CHUNK, 32), F32),
                vmem((LANES, inner), BF16), vmem((LANES, inner), BF16), vmem((3 * n_chunk + 1, 1, inner), F32),
                vmem((n_chunk, CHUNK, CHUNK), F32),
                vmem((tokens, inner), BF16), vmem((tokens, inner), BF16), vmem((tokens, inner), F32),
                vmem((n_chunk + 1, LANES, inner), F32), vmem((n_chunk + 1, LANES, inner), F32),
                vmem((LANES, inner), F32), vmem((LANES, inner), F32), vmem((8, inner), F32), vmem((8, inner), F32),
                vmem((half, d_model), F32), state, state, state, state,
                [vmem((n_chunk, CHUNK, w), BF16) for w in wide], [vmem((n_half, CHUNK, w), BF16) for w in wide],
                dma((8,)), dma((n_grp,)), dma((n_grp,)), dma, dma, dma((n_grp, 2)), dma((n_grp,)),
                dma, dma, dma((n_sp - 1,)), dma((n_sp - 1,)), dma((n_grp, n_half)), dma((n_grp, n_half)),
            ],
            compiler_params=pltpu.CompilerParams(collective_id=0, has_side_effects=True, vmem_limit_bytes=56 * 2 ** 20),
            cost_estimate=pl.CostEstimate(flops=8 * 10 ** 9, bytes_accessed=8 * 10 ** 6, transcendentals=4 * 10 ** 6),
            name='mamba_layer',
        )(x_blk, w_z, w_x, w_bc, w_dt.T, w_out, a_neg, dt_bias, d_skip)

    in_specs = (P(('dp', 'sp'), None), P(None, 'tp'), P(None, 'tp'), P(None, None), P(None, 'tp'), P('tp'), P('tp'), P('tp'), P('tp', None))
    out_specs = P(('dp', 'sp', 'tp'), None)
    return jax.shard_map(device_fn, mesh=mesh, in_specs=in_specs, out_specs=out_specs, check_vma=False)
```

```python
import jax
import jax.numpy as jnp
from jax import lax
from jax.experimental import pallas as pl
from jax.experimental.pallas import tpu as pltpu
from jax.sharding import PartitionSpec as P

MESH = pl.DeviceIdType.MESH
F32 = jnp.float32
BF16 = jnp.bfloat16
LOG2E = 1.4426950408889634

CHUNK = 128
LANES = 128
GROUPS = (1, 2, 3)


def dot(a, b):
    return jnp.dot(a, b, preferred_element_type=F32)


def split3(v):
    hi = v.astype(BF16)
    rest = v - hi.astype(F32)
    mid = rest.astype(BF16)
    return hi, mid, (rest - mid.astype(F32)).astype(BF16)


def softplus(v):
    return jnp.maximum(v, 0.0) + jnp.log1p(jnp.exp(-jnp.abs(v)))


def kernel(dims, x_hbm, wz_hbm, wx_hbm, wbc_hbm, wdt_hbm, wo_hbm, a_s, bias_s, dskip_s, out_ref,
           x_v, wz_v, wx_v, w0_v, wbc_v, wdt_v, wo_own, wo_peer, c_v, bt_v, wide_v, dt_v, ct_v, et_v, cola_v, colx_v, colb_v,
           pick_v, tab_v, gram_v, u_v, z_v, y_v, pf_v, pb_v, hf_v, hb_v, dec_send, dec_recv, acc_v,
           s1_send, s1_recv, s2_send, s2_recv, g_v, g_recv,
           in_sem, s1_ss, s1_rs, dec_ss, dec_rs, s2_ss, s2_rs, wy_ss, wy_rs, wf_ss, wf_rs, g_ss, g_rs):
    tokens, n_head, n_sp = dims
    d_model = x_v.shape[1]
    inner = wx_v.shape[1]
    n_chunk = tokens // CHUNK
    n_half = n_chunk // 2
    half = tokens // 2
    n_grp = len(GROUPS)
    head_dim = inner // n_head
    edge = [LANES * sum(GROUPS[:g]) for g in range(n_grp + 1)]
    wrows = inner // n_sp

    tp = lax.axis_index('tp')
    sp = lax.axis_index('sp')
    core = lax.rem(sp, 2)
    partner = sp + 1 - 2 * core
    other_tp = 1 - tp
    my_base = tp * n_half
    peer_base = other_tp * n_half

    def load(src, dst, i):
        return pltpu.make_async_copy(src, dst, in_sem.at[i])

    ld_bc = load(wbc_hbm, wbc_v, 0)
    ld_dt = load(wdt_hbm, wdt_v, 1)
    ld_x = [load(x_hbm.at[pl.ds(i * half, half)], x_v.at[pl.ds(i * half, half)], 2 + i) for i in range(2)]
    late = pl.ds(LANES, inner - LANES)
    ld_wx = load(wx_hbm.at[:, late], wx_v.at[:, late], 4)
    ld_w0 = load(wx_hbm.at[:, pl.ds(0, LANES)], w0_v.at[:, pl.ds(0, LANES)], 7)
    ld_wz = load(wz_hbm, wz_v, 5)
    ld_wo = load(wo_hbm, wo_own, 6)
    for ld in (ld_dt, ld_x[0], ld_w0, ld_x[1], ld_bc):
        ld.start()

    barrier = pltpu.get_barrier_semaphore()
    for step in range(1, n_sp):
        pl.semaphore_signal(barrier, inc=1, device_id={'sp': lax.rem(sp + step, n_sp)}, device_id_type=MESH)
    pl.semaphore_signal(barrier, inc=1, device_id={'tp': other_tp}, device_id_type=MESH)

    pl.semaphore_wait(barrier, n_sp)

    my_rows = pl.ds(sp * wrows, wrows)
    wy = pltpu.make_async_remote_copy(src_ref=wo_hbm.at[my_rows], dst_ref=wo_peer.at[my_rows], send_sem=wy_ss, recv_sem=wy_rs,
                                      device_id={'tp': other_tp}, device_id_type=MESH)
    wy.start()
    ld_wx.start()

    row_h = lax.broadcasted_iota(jnp.int32, (16, LANES), 0)
    bias_t = jnp.zeros((16, LANES), F32)
    a_t = jnp.zeros((16, LANES), F32)
    for h in range(n_head):
        bias_t = jnp.where(row_h == h, bias_s[h], bias_t)
        a_t = jnp.where(row_h == h, a_s[h] * LOG2E, a_t)
    sq_r = lax.broadcasted_iota(jnp.int32, (CHUNK, LANES), 0)
    sq_c = lax.broadcasted_iota(jnp.int32, (CHUNK, LANES), 1)
    tri = jnp.concatenate([jnp.where(sq_r <= sq_c, 1.0, 0.0), jnp.where(sq_r < sq_c, 1.0, 0.0)], axis=1).astype(BF16)
    diag2 = jnp.where(sq_r == sq_c, 2.0, 1.0)
    ex_r = lax.broadcasted_iota(jnp.int32, (LANES, 2 * inner), 0)
    ex_c = lax.broadcasted_iota(jnp.int32, (LANES, 2 * inner), 1)
    shift = head_dim.bit_length() - 1
    ex_h = (((ex_c >> 8) << 7) + (ex_c & 127)) >> shift
    ex_t = ex_r - ((ex_c & 128) >> 1)
    pick_v[...] = jnp.where(((ex_r & 15) == ex_h) & (ex_t >= 0) & (ex_t < 48), 1.0, 0.0).astype(BF16)
    one_r = lax.broadcasted_iota(jnp.int32, (32, inner), 0)
    e_one = jnp.where(one_r == (lax.broadcasted_iota(jnp.int32, (32, inner), 1) >> shift), 1.0, 0.0).astype(BF16)
    wide_v[...] = jnp.zeros_like(wide_v)
    ld_dt.wait()
    wide_v[0:n_head, :] = wdt_v[...].astype(F32)
    for k in range(d_model // LANES):
        rows = slice(k * LANES, (k + 1) * LANES)
        w0_v[rows, LANES:] = wide_v[:, rows].T.astype(BF16)

    ld_w0.wait()
    for i in range(2):
        ld_x[i].wait()
        rows = slice(i * half, (i + 1) * half)
        first = dot(x_v[rows, :], w0_v[...])
        u_v[rows, :LANES] = first[:, :LANES].astype(BF16)
        for k in range(n_half):
            dt_v[i * n_half + k] = softplus(first[k * CHUNK:(k + 1) * CHUNK, LANES:].T[:16] + bias_t)
    dt_all = dt_v[...].reshape(n_chunk * 16, LANES)
    la_all = (dt_v[...] * a_t[None]).reshape(n_chunk * 16, LANES)
    cum = sum(dot(part, tri) for part in split3(la_all))
    ld_bc.wait()

    def project_bc(i):
        rows = slice(i * half, (i + 1) * half)
        bc_val = dot(x_v[rows, :], wbc_v[...]).astype(BF16)
        c_v[rows, :] = bc_val[:, LANES:]
        for k in range(n_half):
            bt_v[i * n_half + k] = bc_val[k * CHUNK:(k + 1) * CHUNK, :LANES].astype(F32).T.astype(BF16)

    project_bc(0)
    c_log = cum[:, :LANES]
    e_log = cum[:, LANES:]
    ct_v[...] = c_log.reshape(n_chunk, 16, LANES)
    et_v[...] = e_log.reshape(n_chunk, 16, LANES)
    tail = c_log[:, LANES - 1:LANES]
    parts_ef = split3(jnp.exp2(c_log))
    parts_eb = split3(jnp.exp2(tail - e_log))
    parts_wf = split3(jnp.exp2(tail - c_log) * dt_all)
    parts_wb = split3(jnp.exp2(e_log) * dt_all)
    project_bc(1)
    blank = jnp.zeros((16, LANES), F32)

    def row_tile(first, second, c):
        rows = slice(c * 16, (c + 1) * 16)
        tile = [p[rows].astype(F32) for p in first] + [blank] + [p[rows].astype(F32) for p in second] + [blank]
        return jnp.concatenate(tile, axis=0)

    def column_tile(first, second, c):
        return row_tile(first, second, c).T.astype(BF16)

    run = jnp.zeros((1, 32), F32)
    tails, starts, ends = [], [], []
    for c in range(n_chunk):
        rows = slice(c * 16, (c + 1) * 16)
        colb_v[c] = column_tile(parts_wf, parts_wb, c)
        cola_v[c] = row_tile(parts_ef, parts_eb, c)
        col = jnp.concatenate([c_log[rows], e_log[rows]], axis=0).T
        last = col[CHUNK - 1:CHUNK, :]
        tails.append(last)
        starts.append(run)
        run = run + last
        ends.append(run)
    logs = jnp.concatenate(tails + starts + [run - e for e in ends] + [run] * n_chunk, axis=0)
    tab = sum(dot(part, e_one) for part in split3(jnp.exp2(logs)))
    for i in range(3 * n_chunk + 1):
        tab_v[i] = tab[i:i + 1, :]
    dec_send[...] = tab[3 * n_chunk:, :]

    ld_wz.start()
    ld_wo.start()

    def to_partner(g):
        return pltpu.make_async_remote_copy(src_ref=s1_send[g], dst_ref=s1_recv[g], send_sem=s1_ss.at[g], recv_sem=s1_rs.at[g],
                                            device_id={'sp': partner}, device_id_type=MESH)

    def to_chip(g, t):
        return pltpu.make_async_remote_copy(src_ref=s2_send[g], dst_ref=s2_recv[g], send_sem=s2_ss.at[g, t], recv_sem=s2_rs.at[g],
                                            device_id={'sp': 2 - 2 * (sp // 2) + t}, device_id_type=MESH)

    def to_peer(g, k):
        return pltpu.make_async_remote_copy(src_ref=g_v[g].at[peer_base + k], dst_ref=g_recv[g].at[k], send_sem=g_ss.at[g, k],
                                            recv_sem=g_rs.at[g, k], device_id={'tp': other_tp}, device_id_type=MESH)

    def gather(i):
        owner = lax.rem(sp + 2, n_sp) if i == 2 else sp
        block = wo_peer.at[pl.ds(owner * wrows, wrows)]
        target = lax.rem(sp + 2, n_sp) if i == 1 else partner
        return pltpu.make_async_remote_copy(src_ref=block, dst_ref=block, send_sem=wf_ss.at[i], recv_sem=wf_rs.at[i],
                                            device_id={'sp': target}, device_id_type=MESH)

    dec_copy = pltpu.make_async_remote_copy(src_ref=dec_send, dst_ref=dec_recv, send_sem=dec_ss, recv_sem=dec_rs,
                                            device_id={'sp': partner}, device_id_type=MESH)
    dec_copy.start()

    def project_u(g):
        cols = slice(edge[g], edge[g + 1])
        for i in range(2):
            rows = slice(i * half, (i + 1) * half)
            u_v[rows, cols] = dot(x_v[rows, :], wx_v[:, cols]).astype(BF16)

    def states(g):
        for lo in range(edge[g], edge[g + 1], LANES):
            cols = slice(lo, lo + LANES)
            pick = pick_v[:, 2 * lo:2 * lo + 2 * LANES]
            acc = jnp.zeros((LANES, LANES), F32)
            for c in range(n_chunk):
                u_c = u_v[c * CHUNK:(c + 1) * CHUNK, cols].astype(F32)
                w_c = dot(colb_v[c], pick)
                u_w = jnp.concatenate([u_c * w_c[:, :LANES], u_c * w_c[:, LANES:]], axis=1).astype(BF16)
                st = dot(bt_v[c], u_w)
                pf_v[c, :, cols] = acc
                acc = tab_v[c][:, cols] * acc + st[:, :LANES]
                pb_v[c, :, cols] = st[:, LANES:]
            pf_v[n_chunk, :, cols] = acc
            acc = jnp.zeros((LANES, LANES), F32)
            for c in reversed(range(n_chunk)):
                st = pb_v[c, :, cols]
                pb_v[c, :, cols] = acc
                acc = tab_v[c][:, cols] * acc + st
            pb_v[n_chunk, :, cols] = acc
            s1_send[g][:, lo - edge[g]:lo - edge[g] + LANES] = jnp.where(core == 0, pf_v[n_chunk, :, cols], acc).astype(BF16)
        to_partner(g).start()

    sends_far = (sp == 1) | (sp == 2)

    def pass_on(g):
        to_partner(g).wait_recv()

        @pl.when(sends_far)
        def _():
            cols = slice(edge[g], edge[g + 1])
            own = jnp.where(core == 1, pf_v[n_chunk, :, cols], pb_v[n_chunk, :, cols])
            s2_send[g][...] = (own + tab_v[3 * n_chunk][:, cols] * s1_recv[g][...].astype(F32)).astype(BF16)
            to_chip(g, 0).start()
            to_chip(g, 1).start()

    def incoming(g):
        to_chip(g, 0).wait_recv()
        cols = slice(edge[g], edge[g + 1])
        near = s1_recv[g][...].astype(F32)
        far = s2_recv[g][...].astype(F32)
        both = near + dec_recv[0:1, cols] * far
        hf_v[:, cols] = jnp.where(sp == 0, 0.0, jnp.where(sp == 1, near, jnp.where(sp == 2, far, both)))
        hb_v[:, cols] = jnp.where(sp == 3, 0.0, jnp.where(sp == 2, near, jnp.where(sp == 1, far, both)))

    lane = lax.broadcasted_iota(jnp.int32, (CHUNK, LANES), 1)
    low_lane = lane < head_dim
    above = sq_r < sq_c
    below = sq_r > sq_c

    def project_z(g, base):
        cols = slice(edge[g], edge[g + 1])
        rows = pl.ds(pl.multiple_of(base * CHUNK, CHUNK), half)
        z_v[rows, cols] = dot(x_v[rows, :], wz_v[:, cols]).astype(BF16)

    def intra(g, c):
        rows = pl.ds(pl.multiple_of(c * CHUNK, CHUNK), CHUNK)
        gram = gram_v[c]
        for lo in range(edge[g], edge[g + 1], LANES):
            lanes = slice(lo, lo + LANES)
            h0 = lo // head_dim
            u_pair = u_v[rows, lanes]
            weights = []
            for h in (h0, h0 + 1):
                incl = ct_v[c, h:h + 1, :]
                excl = et_v[c, h:h + 1, :]
                gap = jnp.where(above, incl, excl).T - jnp.where(below, incl, excl)
                weights.append((gram * jnp.exp2(jnp.minimum(gap, -gap)) * dt_v[c, h:h + 1, :]).astype(BF16))
            zero = jnp.zeros_like(u_pair)
            u_diag = jnp.concatenate([jnp.where(low_lane, u_pair, zero), jnp.where(low_lane, zero, u_pair)], axis=0)
            skip = jnp.where(low_lane[:1], 2.0 * dskip_s[h0], 2.0 * dskip_s[h0 + 1])
            y_v[rows, lanes] = dot(jnp.concatenate(weights, axis=1), u_diag) + skip * u_pair.astype(F32)

    def finish(g, c):
        rows = pl.ds(pl.multiple_of(c * CHUNK, CHUNK), CHUNK)
        c_mat = c_v[rows, :]
        for lo in range(edge[g], edge[g + 1], LANES):
            cols = slice(lo, lo + LANES)
            in_f = pf_v[c, :, cols] + tab_v[n_chunk + c][:, cols] * hf_v[:, cols]
            in_b = pb_v[c, :, cols] + tab_v[2 * n_chunk + c][:, cols] * hb_v[:, cols]
            w_c = dot(colx_v[c], pick_v[:, 2 * lo:2 * lo + 2 * LANES])
            y_in = w_c * dot(c_mat, jnp.concatenate([in_f, in_b], axis=1).astype(BF16))
            y = y_v[rows, cols] + y_in[:, :LANES] + y_in[:, LANES:]
            hz = 0.5 * z_v[rows, cols].astype(F32)
            g_v[g][c, :, lo - edge[g]:lo - edge[g] + LANES] = (y * (hz + hz * jnp.tanh(hz))).astype(BF16)

    def gram_part(base):
        for k in range(n_half):
            c = base + k
            colx_v[c] = cola_v[c].T.astype(BF16)
            gram_v[c] = dot(c_v[pl.ds(pl.multiple_of(c * CHUNK, CHUNK), CHUNK), :], bt_v[c]) * diag2

    def send_finished(g):
        incoming(g)
        for k in range(n_half):
            finish(g, peer_base + k)
            to_peer(g, k).start()

    states(0)
    gram_part(peer_base)
    ld_wx.wait()
    project_u(1)
    pass_on(0)
    states(1)
    ld_wz.wait()
    project_z(0, peer_base)
    for k in range(n_half):
        intra(0, peer_base + k)
    pass_on(1)
    project_u(2)
    dec_copy.wait_recv()
    send_finished(0)
    states(2)
    project_z(1, peer_base)
    for k in range(n_half):
        intra(1, peer_base + k)
    pass_on(2)
    send_finished(1)
    wy.wait_recv()
    gather(0).start()
    gather(1).start()
    project_z(2, peer_base)
    for k in range(n_half):
        intra(2, peer_base + k)
    send_finished(2)

    gram_part(my_base)
    for g in range(n_grp):
        project_z(g, my_base)
        for k in range(n_half):
            intra(g, my_base + k)
        for k in range(n_half):
            finish(g, my_base + k)
    ld_wo.wait()
    my_tokens = pl.ds(pl.multiple_of(my_base * CHUNK, CHUNK), half)
    acc_v[...] = x_v[my_tokens, :].astype(F32)
    for g in range(n_grp):
        mine = g_v[g][pl.ds(my_base, n_half)].reshape(half, edge[g + 1] - edge[g])
        acc_v[...] += dot(mine, wo_own[edge[g]:edge[g + 1], :])
    gather(1).wait_recv()
    gather(2).start()
    gather(0).wait_recv()
    gather(2).wait_recv()
    for g in range(n_grp):
        w_g = wo_peer[edge[g]:edge[g + 1], :]
        for k in range(n_half):
            to_peer(g, k).wait_recv()
            rows = slice(k * CHUNK, (k + 1) * CHUNK)
            val = acc_v[rows, :] + dot(g_recv[g][k], w_g)
            if g < n_grp - 1:
                acc_v[rows, :] = val
            else:
                out_ref[rows, :] = val.astype(BF16)

    wy.wait_send()
    dec_copy.wait_send()
    for i in range(3):
        gather(i).wait_send()
    for g in range(n_grp):
        to_partner(g).wait_send()

        @pl.when(sends_far)
        def _():
            to_chip(g, 0).wait_send()
            to_chip(g, 1).wait_send()
        for k in range(n_half):
            to_peer(g, k).wait_send()


def solution(mesh):
    n_sp = mesh.shape['sp']

    def device_fn(x_blk, w_z, w_x, w_bc, w_dt, a_neg, dt_bias, d_skip, w_out):
        tokens, d_model = x_blk.shape
        n_head = a_neg.shape[0]
        inner = w_x.shape[1]
        half = tokens // 2
        n_chunk = tokens // CHUNK
        n_half = n_chunk // 2
        n_grp = len(GROUPS)
        wide = [LANES * p for p in GROUPS]
        vmem = pltpu.VMEM
        dma = pltpu.SemaphoreType.DMA
        state = [vmem((LANES, w), BF16) for w in wide]
        hbm = pl.BlockSpec(memory_space=pltpu.HBM)
        smem = pl.BlockSpec(memory_space=pltpu.SMEM)

        def body(*refs):
            kernel((tokens, n_head, n_sp), *refs)

        return pl.pallas_call(
            body,
            out_shape=pltpu.VMEM((half, d_model), BF16),
            in_specs=[hbm] * 6 + [smem] * 3,
            out_specs=pl.BlockSpec(memory_space=pltpu.VMEM),
            scratch_shapes=[
                vmem((tokens, d_model), BF16), vmem((d_model, inner), BF16), vmem((d_model, inner), BF16), vmem((d_model, 2 * LANES), BF16),
                vmem(w_bc.shape, BF16), vmem(w_dt.shape[::-1], BF16), vmem((inner, d_model), BF16), vmem((inner, d_model), BF16),
                vmem((tokens, LANES), BF16), vmem((n_chunk, LANES, CHUNK), BF16), vmem((LANES, d_model), F32),
                vmem((n_chunk, 16, LANES), F32), vmem((n_chunk, 16, LANES), F32), vmem((n_chunk, 16, LANES), F32),
                vmem((n_chunk, LANES, CHUNK), F32), vmem((n_chunk, CHUNK, LANES), BF16), vmem((n_chunk, CHUNK, LANES), BF16),
                vmem((LANES, 2 * inner), BF16), vmem((3 * n_chunk + 1, 1, inner), F32),
                vmem((n_chunk, CHUNK, CHUNK), F32),
                vmem((tokens, inner), BF16), vmem((tokens, inner), BF16), vmem((tokens, inner), F32),
                vmem((n_chunk + 1, LANES, inner), F32), vmem((n_chunk + 1, LANES, inner), F32),
                vmem((LANES, inner), F32), vmem((LANES, inner), F32), vmem((8, inner), F32), vmem((8, inner), F32),
                vmem((half, d_model), F32), state, state, state, state,
                [vmem((n_chunk, CHUNK, w), BF16) for w in wide], [vmem((n_half, CHUNK, w), BF16) for w in wide],
                dma((8,)), dma((n_grp,)), dma((n_grp,)), dma, dma, dma((n_grp, 2)), dma((n_grp,)),
                dma, dma, dma((3,)), dma((3,)), dma((n_grp, n_half)), dma((n_grp, n_half)),
            ],
            compiler_params=pltpu.CompilerParams(collective_id=0, has_side_effects=True, vmem_limit_bytes=56 * 2 ** 20),
            cost_estimate=pl.CostEstimate(flops=8 * 10 ** 9, bytes_accessed=8 * 10 ** 6, transcendentals=4 * 10 ** 6),
            name='mamba_layer',
        )(x_blk, w_z, w_x, w_bc, w_dt.T, w_out, a_neg, dt_bias, d_skip)

    in_specs = (P(('dp', 'sp'), None), P(None, 'tp'), P(None, 'tp'), P(None, None), P(None, 'tp'), P('tp'), P('tp'), P('tp'), P('tp', None))
    out_specs = P(('dp', 'sp', 'tp'), None)
    return jax.shard_map(device_fn, mesh=mesh, in_specs=in_specs, out_specs=out_specs, check_vma=False)
```

```python
import jax
import jax.numpy as jnp
from jax import lax
from jax.experimental import pallas as pl
from jax.experimental.pallas import tpu as pltpu
from jax.sharding import PartitionSpec as P

MESH = pl.DeviceIdType.MESH
F32 = jnp.float32
BF16 = jnp.bfloat16
LOG2E = 1.4426950408889634

CHUNK = 128
LANES = 128
GROUPS = (1, 2, 3)


def dot(a, b):
    return jnp.dot(a, b, preferred_element_type=F32)


def split3(v):
    hi = v.astype(BF16)
    rest = v - hi.astype(F32)
    mid = rest.astype(BF16)
    return hi, mid, (rest - mid.astype(F32)).astype(BF16)


def softplus(v):
    return jnp.maximum(v, 0.0) + jnp.log1p(jnp.exp(-jnp.abs(v)))


def kernel(dims, x_hbm, wz_hbm, wx_hbm, wbc_hbm, wdt_hbm, wo_hbm, a_s, bias_s, dskip_s, out_ref,
           x_v, wz_v, wx_v, w0_v, wbc_v, wdt_v, wo_own, wo_peer, c_v, bt_v, wide_v, dt_v, ct_v, et_v, cola_v, colx_v, colb_v,
           pick_v, tab_v, gram_v, u_v, z_v, y_v, pf_v, pb_v, hf_v, hb_v, dec_send, dec_recv, acc_v,
           s1_send, s1_recv, s2_send, s2_recv, g_v, g_recv,
           in_sem, s1_ss, s1_rs, dec_ss, dec_rs, s2_ss, s2_rs, wy_ss, wy_rs, wf_ss, wf_rs, g_ss, g_rs):
    tokens, n_head, n_sp = dims
    d_model = x_v.shape[1]
    inner = wx_v.shape[1]
    n_chunk = tokens // CHUNK
    n_half = n_chunk // 2
    half = tokens // 2
    n_grp = len(GROUPS)
    head_dim = inner // n_head
    edge = [LANES * sum(GROUPS[:g]) for g in range(n_grp + 1)]
    wrows = inner // n_sp

    tp = lax.axis_index('tp')
    sp = lax.axis_index('sp')
    core = lax.rem(sp, 2)
    partner = sp + 1 - 2 * core
    other_tp = 1 - tp
    my_base = tp * n_half
    peer_base = other_tp * n_half

    def load(src, dst, i):
        return pltpu.make_async_copy(src, dst, in_sem.at[i])

    ld_bc = load(wbc_hbm, wbc_v, 0)
    ld_dt = load(wdt_hbm, wdt_v, 1)
    ld_x = [load(x_hbm.at[pl.ds(i * half, half)], x_v.at[pl.ds(i * half, half)], 2 + i) for i in range(2)]
    late = pl.ds(LANES, inner - LANES)
    ld_wx = load(wx_hbm.at[:, late], wx_v.at[:, late], 4)
    ld_w0 = load(wx_hbm.at[:, pl.ds(0, LANES)], w0_v.at[:, pl.ds(0, LANES)], 7)
    ld_wz = load(wz_hbm, wz_v, 5)
    ld_wo = load(wo_hbm, wo_own, 6)
    for ld in (ld_dt, ld_x[0], ld_w0, ld_x[1], ld_bc):
        ld.start()

    barrier = pltpu.get_barrier_semaphore()
    for step in range(1, n_sp):
        pl.semaphore_signal(barrier, inc=1, device_id={'sp': lax.rem(sp + step, n_sp)}, device_id_type=MESH)
    pl.semaphore_signal(barrier, inc=1, device_id={'tp': other_tp}, device_id_type=MESH)

    pl.semaphore_wait(barrier, n_sp)

    my_rows = pl.ds(sp * wrows, wrows)
    wy = pltpu.make_async_remote_copy(src_ref=wo_hbm.at[my_rows], dst_ref=wo_peer.at[my_rows], send_sem=wy_ss, recv_sem=wy_rs,
                                      device_id={'tp': other_tp}, device_id_type=MESH)
    wy.start()
    ld_wx.start()

    row_h = lax.broadcasted_iota(jnp.int32, (16, LANES), 0)
    bias_t = jnp.zeros((16, LANES), F32)
    a_t = jnp.zeros((16, LANES), F32)
    for h in range(n_head):
        bias_t = jnp.where(row_h == h, bias_s[h], bias_t)
        a_t = jnp.where(row_h == h, a_s[h] * LOG2E, a_t)
    sq_r = lax.broadcasted_iota(jnp.int32, (CHUNK, LANES), 0)
    sq_c = lax.broadcasted_iota(jnp.int32, (CHUNK, LANES), 1)
    tri = jnp.concatenate([jnp.where(sq_r <= sq_c, 1.0, 0.0), jnp.where(sq_r < sq_c, 1.0, 0.0)], axis=1).astype(BF16)
    diag2 = jnp.where(sq_r == sq_c, 2.0, 1.0)
    ex_r = lax.broadcasted_iota(jnp.int32, (LANES, 2 * inner), 0)
    ex_c = lax.broadcasted_iota(jnp.int32, (LANES, 2 * inner), 1)
    shift = head_dim.bit_length() - 1
    ex_h = (((ex_c >> 8) << 7) + (ex_c & 127)) >> shift
    ex_t = ex_r - ((ex_c & 128) >> 1)
    pick_v[...] = jnp.where(((ex_r & 15) == ex_h) & (ex_t >= 0) & (ex_t < 48), 1.0, 0.0).astype(BF16)
    one_r = lax.broadcasted_iota(jnp.int32, (32, inner), 0)
    e_one = jnp.where(one_r == (lax.broadcasted_iota(jnp.int32, (32, inner), 1) >> shift), 1.0, 0.0).astype(BF16)
    wide_v[...] = jnp.zeros_like(wide_v)
    ld_dt.wait()
    wide_v[0:n_head, :] = wdt_v[...].astype(F32)
    for k in range(d_model // LANES):
        rows = slice(k * LANES, (k + 1) * LANES)
        w0_v[rows, LANES:] = wide_v[:, rows].T.astype(BF16)

    ld_w0.wait()
    for i in range(2):
        ld_x[i].wait()
        rows = slice(i * half, (i + 1) * half)
        first = dot(x_v[rows, :], w0_v[...])
        u_v[rows, :LANES] = first[:, :LANES].astype(BF16)
        for k in range(n_half):
            dt_v[i * n_half + k] = softplus(first[k * CHUNK:(k + 1) * CHUNK, LANES:].T[:16] + bias_t)
    dt_all = dt_v[...].reshape(n_chunk * 16, LANES)
    la_all = (dt_v[...] * a_t[None]).reshape(n_chunk * 16, LANES)
    cum = sum(dot(part, tri) for part in split3(la_all))
    ld_bc.wait()

    def project_bc(i):
        rows = slice(i * half, (i + 1) * half)
        bc_val = dot(x_v[rows, :], wbc_v[...]).astype(BF16)
        c_v[rows, :] = bc_val[:, LANES:]
        for k in range(n_half):
            bt_v[i * n_half + k] = bc_val[k * CHUNK:(k + 1) * CHUNK, :LANES].astype(F32).T.astype(BF16)

    project_bc(0)
    c_log = cum[:, :LANES]
    e_log = cum[:, LANES:]
    ct_v[...] = c_log.reshape(n_chunk, 16, LANES)
    et_v[...] = e_log.reshape(n_chunk, 16, LANES)
    tail = c_log[:, LANES - 1:LANES]
    parts_ef = split3(jnp.exp2(c_log))
    parts_eb = split3(jnp.exp2(tail - e_log))
    parts_wf = split3(jnp.exp2(tail - c_log) * dt_all)
    parts_wb = split3(jnp.exp2(e_log) * dt_all)
    project_bc(1)
    blank = jnp.zeros((16, LANES), F32)

    def row_tile(first, second, c):
        rows = slice(c * 16, (c + 1) * 16)
        tile = [p[rows].astype(F32) for p in first] + [blank] + [p[rows].astype(F32) for p in second] + [blank]
        return jnp.concatenate(tile, axis=0)

    def column_tile(first, second, c):
        return row_tile(first, second, c).T.astype(BF16)

    run = jnp.zeros((1, 32), F32)
    tails, starts, ends = [], [], []
    for c in range(n_chunk):
        rows = slice(c * 16, (c + 1) * 16)
        colb_v[c] = column_tile(parts_wf, parts_wb, c)
        cola_v[c] = row_tile(parts_ef, parts_eb, c)
        col = jnp.concatenate([c_log[rows], e_log[rows]], axis=0).T
        last = col[CHUNK - 1:CHUNK, :]
        tails.append(last)
        starts.append(run)
        run = run + last
        ends.append(run)
    logs = jnp.concatenate(tails + starts + [run - e for e in ends] + [run] * n_chunk, axis=0)
    tab = sum(dot(part, e_one) for part in split3(jnp.exp2(logs)))
    for i in range(3 * n_chunk + 1):
        tab_v[i] = tab[i:i + 1, :]
    dec_send[...] = tab[3 * n_chunk:, :]

    ld_wz.start()
    ld_wo.start()

    def to_partner(g):
        return pltpu.make_async_remote_copy(src_ref=s1_send[g], dst_ref=s1_recv[g], send_sem=s1_ss.at[g], recv_sem=s1_rs.at[g],
                                            device_id={'sp': partner}, device_id_type=MESH)

    def to_chip(g, t):
        return pltpu.make_async_remote_copy(src_ref=s2_send[g], dst_ref=s2_recv[g], send_sem=s2_ss.at[g, t], recv_sem=s2_rs.at[g],
                                            device_id={'sp': 2 - 2 * (sp // 2) + t}, device_id_type=MESH)

    def to_peer(g, k):
        return pltpu.make_async_remote_copy(src_ref=g_v[g].at[peer_base + k], dst_ref=g_recv[g].at[k], send_sem=g_ss.at[g, k],
                                            recv_sem=g_rs.at[g, k], device_id={'tp': other_tp}, device_id_type=MESH)

    def gather(i):
        owner = lax.rem(sp + 2, n_sp) if i == 2 else sp
        block = wo_peer.at[pl.ds(owner * wrows, wrows)]
        target = lax.rem(sp + 2, n_sp) if i == 1 else partner
        return pltpu.make_async_remote_copy(src_ref=block, dst_ref=block, send_sem=wf_ss.at[i], recv_sem=wf_rs.at[i],
                                            device_id={'sp': target}, device_id_type=MESH)

    dec_copy = pltpu.make_async_remote_copy(src_ref=dec_send, dst_ref=dec_recv, send_sem=dec_ss, recv_sem=dec_rs,
                                            device_id={'sp': partner}, device_id_type=MESH)
    dec_copy.start()

    def project_u(g):
        cols = slice(edge[g], edge[g + 1])
        for i in range(2):
            rows = slice(i * half, (i + 1) * half)
            u_v[rows, cols] = dot(x_v[rows, :], wx_v[:, cols]).astype(BF16)

    def states(g):
        for lo in range(edge[g], edge[g + 1], LANES):
            cols = slice(lo, lo + LANES)
            pick = pick_v[:, 2 * lo:2 * lo + 2 * LANES]
            acc = jnp.zeros((LANES, LANES), F32)
            for c in range(n_chunk):
                u_c = u_v[c * CHUNK:(c + 1) * CHUNK, cols].astype(F32)
                w_c = dot(colb_v[c], pick)
                u_w = jnp.concatenate([u_c * w_c[:, :LANES], u_c * w_c[:, LANES:]], axis=1).astype(BF16)
                st = dot(bt_v[c], u_w)
                pf_v[c, :, cols] = acc
                acc = tab_v[c][:, cols] * acc + st[:, :LANES]
                pb_v[c, :, cols] = st[:, LANES:]
            pf_v[n_chunk, :, cols] = acc
            acc = jnp.zeros((LANES, LANES), F32)
            for c in reversed(range(n_chunk)):
                st = pb_v[c, :, cols]
                pb_v[c, :, cols] = acc
                acc = tab_v[c][:, cols] * acc + st
            pb_v[n_chunk, :, cols] = acc
            s1_send[g][:, lo - edge[g]:lo - edge[g] + LANES] = jnp.where(core == 0, pf_v[n_chunk, :, cols], acc).astype(BF16)
        to_partner(g).start()

    sends_far = (sp == 1) | (sp == 2)

    def pass_on(g):
        to_partner(g).wait_recv()

        @pl.when(sends_far)
        def _():
            cols = slice(edge[g], edge[g + 1])
            own = jnp.where(core == 1, pf_v[n_chunk, :, cols], pb_v[n_chunk, :, cols])
            s2_send[g][...] = (own + tab_v[3 * n_chunk][:, cols] * s1_recv[g][...].astype(F32)).astype(BF16)
            to_chip(g, 0).start()
            to_chip(g, 1).start()

    def incoming(g):
        to_chip(g, 0).wait_recv()
        cols = slice(edge[g], edge[g + 1])
        near = s1_recv[g][...].astype(F32)
        far = s2_recv[g][...].astype(F32)
        both = near + dec_recv[0:1, cols] * far
        hf_v[:, cols] = jnp.where(sp == 0, 0.0, jnp.where(sp == 1, near, jnp.where(sp == 2, far, both)))
        hb_v[:, cols] = jnp.where(sp == 3, 0.0, jnp.where(sp == 2, near, jnp.where(sp == 1, far, both)))

    lane = lax.broadcasted_iota(jnp.int32, (CHUNK, LANES), 1)
    low_lane = lane < head_dim
    above = sq_r < sq_c
    below = sq_r > sq_c

    def project_z(g, base):
        cols = slice(edge[g], edge[g + 1])
        rows = pl.ds(pl.multiple_of(base * CHUNK, CHUNK), half)
        z_v[rows, cols] = dot(x_v[rows, :], wz_v[:, cols]).astype(BF16)

    def intra(g, c):
        rows = pl.ds(pl.multiple_of(c * CHUNK, CHUNK), CHUNK)
        gram = gram_v[c]
        for lo in range(edge[g], edge[g + 1], LANES):
            lanes = slice(lo, lo + LANES)
            h0 = lo // head_dim
            u_pair = u_v[rows, lanes]
            weights = []
            for h in (h0, h0 + 1):
                incl = ct_v[c, h:h + 1, :]
                excl = et_v[c, h:h + 1, :]
                gap = jnp.where(above, incl, excl).T - jnp.where(below, incl, excl)
                weights.append((gram * jnp.exp2(jnp.minimum(gap, -gap)) * dt_v[c, h:h + 1, :]).astype(BF16))
            zero = jnp.zeros_like(u_pair)
            u_diag = jnp.concatenate([jnp.where(low_lane, u_pair, zero), jnp.where(low_lane, zero, u_pair)], axis=0)
            skip = jnp.where(low_lane[:1], 2.0 * dskip_s[h0], 2.0 * dskip_s[h0 + 1])
            y_v[rows, lanes] = dot(jnp.concatenate(weights, axis=1), u_diag) + skip * u_pair.astype(F32)

    def finish(g, c):
        rows = pl.ds(pl.multiple_of(c * CHUNK, CHUNK), CHUNK)
        c_mat = c_v[rows, :]
        for lo in range(edge[g], edge[g + 1], LANES):
            cols = slice(lo, lo + LANES)
            in_f = pf_v[c, :, cols] + tab_v[n_chunk + c][:, cols] * hf_v[:, cols]
            in_b = pb_v[c, :, cols] + tab_v[2 * n_chunk + c][:, cols] * hb_v[:, cols]
            w_c = dot(colx_v[c], pick_v[:, 2 * lo:2 * lo + 2 * LANES])
            y_in = w_c * dot(c_mat, jnp.concatenate([in_f, in_b], axis=1).astype(BF16))
            y = y_v[rows, cols] + y_in[:, :LANES] + y_in[:, LANES:]
            hz = 0.5 * z_v[rows, cols].astype(F32)
            g_v[g][c, :, lo - edge[g]:lo - edge[g] + LANES] = (y * (hz + hz * jnp.tanh(hz))).astype(BF16)

    def gram_part(base):
        for k in range(n_half):
            c = base + k
            colx_v[c] = cola_v[c].T.astype(BF16)
            gram_v[c] = dot(c_v[pl.ds(pl.multiple_of(c * CHUNK, CHUNK), CHUNK), :], bt_v[c]) * diag2

    def send_finished(g):
        incoming(g)
        for k in range(n_half):
            finish(g, peer_base + k)
            to_peer(g, k).start()

    states(0)
    ld_wx.wait()
    project_u(1)
    pass_on(0)
    gram_part(peer_base)
    states(1)
    ld_wz.wait()
    project_z(0, peer_base)
    for k in range(n_half):
        intra(0, peer_base + k)
    pass_on(1)
    dec_copy.wait_recv()
    send_finished(0)
    project_u(2)
    states(2)
    project_z(1, peer_base)
    for k in range(n_half):
        intra(1, peer_base + k)
    pass_on(2)
    send_finished(1)
    wy.wait_recv()
    gather(0).start()
    gather(1).start()
    project_z(2, peer_base)
    for k in range(n_half):
        intra(2, peer_base + k)
    send_finished(2)

    gram_part(my_base)
    for g in range(n_grp):
        project_z(g, my_base)
        for k in range(n_half):
            intra(g, my_base + k)
        for k in range(n_half):
            finish(g, my_base + k)
    ld_wo.wait()
    my_tokens = pl.ds(pl.multiple_of(my_base * CHUNK, CHUNK), half)
    acc_v[...] = x_v[my_tokens, :].astype(F32)
    for g in range(n_grp):
        mine = g_v[g][pl.ds(my_base, n_half)].reshape(half, edge[g + 1] - edge[g])
        acc_v[...] += dot(mine, wo_own[edge[g]:edge[g + 1], :])
    gather(1).wait_recv()
    gather(2).start()
    gather(0).wait_recv()
    gather(2).wait_recv()
    for g in range(n_grp):
        w_g = wo_peer[edge[g]:edge[g + 1], :]
        for k in range(n_half):
            to_peer(g, k).wait_recv()
            rows = slice(k * CHUNK, (k + 1) * CHUNK)
            val = acc_v[rows, :] + dot(g_recv[g][k], w_g)
            if g < n_grp - 1:
                acc_v[rows, :] = val
            else:
                out_ref[rows, :] = val.astype(BF16)

    wy.wait_send()
    dec_copy.wait_send()
    for i in range(3):
        gather(i).wait_send()
    for g in range(n_grp):
        to_partner(g).wait_send()

        @pl.when(sends_far)
        def _():
            to_chip(g, 0).wait_send()
            to_chip(g, 1).wait_send()
        for k in range(n_half):
            to_peer(g, k).wait_send()


def solution(mesh):
    n_sp = mesh.shape['sp']

    def device_fn(x_blk, w_z, w_x, w_bc, w_dt, a_neg, dt_bias, d_skip, w_out):
        tokens, d_model = x_blk.shape
        n_head = a_neg.shape[0]
        inner = w_x.shape[1]
        half = tokens // 2
        n_chunk = tokens // CHUNK
        n_half = n_chunk // 2
        n_grp = len(GROUPS)
        wide = [LANES * p for p in GROUPS]
        vmem = pltpu.VMEM
        dma = pltpu.SemaphoreType.DMA
        state = [vmem((LANES, w), BF16) for w in wide]
        hbm = pl.BlockSpec(memory_space=pltpu.HBM)
        smem = pl.BlockSpec(memory_space=pltpu.SMEM)

        def body(*refs):
            kernel((tokens, n_head, n_sp), *refs)

        return pl.pallas_call(
            body,
            out_shape=pltpu.VMEM((half, d_model), BF16),
            in_specs=[hbm] * 6 + [smem] * 3,
            out_specs=pl.BlockSpec(memory_space=pltpu.VMEM),
            scratch_shapes=[
                vmem((tokens, d_model), BF16), vmem((d_model, inner), BF16), vmem((d_model, inner), BF16), vmem((d_model, 2 * LANES), BF16),
                vmem(w_bc.shape, BF16), vmem(w_dt.shape[::-1], BF16), vmem((inner, d_model), BF16), vmem((inner, d_model), BF16),
                vmem((tokens, LANES), BF16), vmem((n_chunk, LANES, CHUNK), BF16), vmem((LANES, d_model), F32),
                vmem((n_chunk, 16, LANES), F32), vmem((n_chunk, 16, LANES), F32), vmem((n_chunk, 16, LANES), F32),
                vmem((n_chunk, LANES, CHUNK), F32), vmem((n_chunk, CHUNK, LANES), BF16), vmem((n_chunk, CHUNK, LANES), BF16),
                vmem((LANES, 2 * inner), BF16), vmem((3 * n_chunk + 1, 1, inner), F32),
                vmem((n_chunk, CHUNK, CHUNK), F32),
                vmem((tokens, inner), BF16), vmem((tokens, inner), BF16), vmem((tokens, inner), F32),
                vmem((n_chunk + 1, LANES, inner), F32), vmem((n_chunk + 1, LANES, inner), F32),
                vmem((LANES, inner), F32), vmem((LANES, inner), F32), vmem((8, inner), F32), vmem((8, inner), F32),
                vmem((half, d_model), F32), state, state, state, state,
                [vmem((n_chunk, CHUNK, w), BF16) for w in wide], [vmem((n_half, CHUNK, w), BF16) for w in wide],
                dma((8,)), dma((n_grp,)), dma((n_grp,)), dma, dma, dma((n_grp, 2)), dma((n_grp,)),
                dma, dma, dma((3,)), dma((3,)), dma((n_grp, n_half)), dma((n_grp, n_half)),
            ],
            compiler_params=pltpu.CompilerParams(collective_id=0, has_side_effects=True, vmem_limit_bytes=56 * 2 ** 20),
            cost_estimate=pl.CostEstimate(flops=8 * 10 ** 9, bytes_accessed=8 * 10 ** 6, transcendentals=4 * 10 ** 6),
            name='mamba_layer',
        )(x_blk, w_z, w_x, w_bc, w_dt.T, w_out, a_neg, dt_bias, d_skip)

    in_specs = (P(('dp', 'sp'), None), P(None, 'tp'), P(None, 'tp'), P(None, None), P(None, 'tp'), P('tp'), P('tp'), P('tp'), P('tp', None))
    out_specs = P(('dp', 'sp', 'tp'), None)
    return jax.shard_map(device_fn, mesh=mesh, in_specs=in_specs, out_specs=out_specs, check_vma=False)
```

```python
import jax
import jax.numpy as jnp
from jax import lax
from jax.experimental import pallas as pl
from jax.experimental.pallas import tpu as pltpu
from jax.sharding import PartitionSpec as P

MESH = pl.DeviceIdType.MESH
F32 = jnp.float32
BF16 = jnp.bfloat16
LOG2E = 1.4426950408889634

CHUNK = 128
LANES = 128
GROUPS = (1, 2, 3)


def dot(a, b):
    return jnp.dot(a, b, preferred_element_type=F32)


def split3(v):
    hi = v.astype(BF16)
    rest = v - hi.astype(F32)
    mid = rest.astype(BF16)
    return hi, mid, (rest - mid.astype(F32)).astype(BF16)


def softplus(v):
    return jnp.maximum(v, 0.0) + jnp.log1p(jnp.exp(-jnp.abs(v)))


def kernel(dims, x_hbm, wz_hbm, wx_hbm, wbc_hbm, wdt_hbm, wo_hbm, a_s, bias_s, dskip_s, out_ref,
           x_v, wz_v, wx_v, w0_v, wbc_v, wdt_v, wo_own, wo_peer, c_v, bt_v, wide_v, dt_v, ct_v, et_v, cola_v, colx_v, colb_v,
           pick_v, tab_v, gram_v, u_v, z_v, y_v, pf_v, pb_v, hf_v, hb_v, dec_send, dec_recv, acc_v,
           s1_send, s1_recv, s2_send, s2_recv, g_v, g_recv,
           in_sem, s1_ss, s1_rs, dec_ss, dec_rs, s2_ss, s2_rs, wy_ss, wy_rs, wf_ss, wf_rs, g_ss, g_rs):
    tokens, n_head, n_sp = dims
    d_model = x_v.shape[1]
    inner = wx_v.shape[1]
    n_chunk = tokens // CHUNK
    n_half = n_chunk // 2
    half = tokens // 2
    n_grp = len(GROUPS)
    head_dim = inner // n_head
    edge = [LANES * sum(GROUPS[:g]) for g in range(n_grp + 1)]
    wrows = inner // n_sp

    tp = lax.axis_index('tp')
    sp = lax.axis_index('sp')
    core = lax.rem(sp, 2)
    partner = sp + 1 - 2 * core
    other_tp = 1 - tp
    my_base = tp * n_half
    peer_base = other_tp * n_half

    def load(src, dst, i):
        return pltpu.make_async_copy(src, dst, in_sem.at[i])

    ld_bc = load(wbc_hbm, wbc_v, 0)
    ld_dt = load(wdt_hbm, wdt_v, 1)
    ld_x = [load(x_hbm.at[pl.ds(i * half, half)], x_v.at[pl.ds(i * half, half)], 2 + i) for i in range(2)]
    late = pl.ds(LANES, inner - LANES)
    ld_wx = load(wx_hbm.at[:, late], wx_v.at[:, late], 4)
    ld_w0 = load(wx_hbm.at[:, pl.ds(0, LANES)], w0_v.at[:, pl.ds(0, LANES)], 7)
    ld_wz = load(wz_hbm, wz_v, 5)
    ld_wo = load(wo_hbm, wo_own, 6)
    for ld in (ld_dt, ld_x[0], ld_w0, ld_x[1], ld_bc):
        ld.start()

    barrier = pltpu.get_barrier_semaphore()
    for step in range(1, n_sp):
        pl.semaphore_signal(barrier, inc=1, device_id={'sp': lax.rem(sp + step, n_sp)}, device_id_type=MESH)
    pl.semaphore_signal(barrier, inc=1, device_id={'tp': other_tp}, device_id_type=MESH)

    pl.semaphore_wait(barrier, n_sp)

    my_rows = pl.ds(sp * wrows, wrows)
    wy = pltpu.make_async_remote_copy(src_ref=wo_hbm.at[my_rows], dst_ref=wo_peer.at[my_rows], send_sem=wy_ss, recv_sem=wy_rs,
                                      device_id={'tp': other_tp}, device_id_type=MESH)
    wy.start()
    ld_wx.start()

    row_h = lax.broadcasted_iota(jnp.int32, (16, LANES), 0)
    bias_t = jnp.zeros((16, LANES), F32)
    a_t = jnp.zeros((16, LANES), F32)
    for h in range(n_head):
        bias_t = jnp.where(row_h == h, bias_s[h], bias_t)
        a_t = jnp.where(row_h == h, a_s[h] * LOG2E, a_t)
    sq_r = lax.broadcasted_iota(jnp.int32, (CHUNK, LANES), 0)
    sq_c = lax.broadcasted_iota(jnp.int32, (CHUNK, LANES), 1)
    tri = jnp.concatenate([jnp.where(sq_r <= sq_c, 1.0, 0.0), jnp.where(sq_r < sq_c, 1.0, 0.0)], axis=1).astype(BF16)
    diag2 = jnp.where(sq_r == sq_c, 2.0, 1.0)
    ex_r = lax.broadcasted_iota(jnp.int32, (LANES, 2 * inner), 0)
    ex_c = lax.broadcasted_iota(jnp.int32, (LANES, 2 * inner), 1)
    shift = head_dim.bit_length() - 1
    ex_h = (((ex_c >> 8) << 7) + (ex_c & 127)) >> shift
    ex_t = ex_r - ((ex_c & 128) >> 1)
    pick_v[...] = jnp.where(((ex_r & 15) == ex_h) & (ex_t >= 0) & (ex_t < 48), 1.0, 0.0).astype(BF16)
    one_r = lax.broadcasted_iota(jnp.int32, (32, inner), 0)
    e_one = jnp.where(one_r == (lax.broadcasted_iota(jnp.int32, (32, inner), 1) >> shift), 1.0, 0.0).astype(BF16)
    wide_v[...] = jnp.zeros_like(wide_v)
    ld_dt.wait()
    wide_v[0:n_head, :] = wdt_v[...].astype(F32)
    for k in range(d_model // LANES):
        rows = slice(k * LANES, (k + 1) * LANES)
        w0_v[rows, LANES:] = wide_v[:, rows].T.astype(BF16)

    ld_w0.wait()
    for i in range(2):
        ld_x[i].wait()
        rows = slice(i * half, (i + 1) * half)
        first = dot(x_v[rows, :], w0_v[...])
        u_v[rows, :LANES] = first[:, :LANES].astype(BF16)
        for k in range(n_half):
            dt_v[i * n_half + k] = softplus(first[k * CHUNK:(k + 1) * CHUNK, LANES:].T[:16] + bias_t)
    dt_all = dt_v[...].reshape(n_chunk * 16, LANES)
    la_all = (dt_v[...] * a_t[None]).reshape(n_chunk * 16, LANES)
    cum = sum(dot(part, tri) for part in split3(la_all))
    ld_bc.wait()

    def project_bc(i):
        rows = slice(i * half, (i + 1) * half)
        bc_val = dot(x_v[rows, :], wbc_v[...]).astype(BF16)
        c_v[rows, :] = bc_val[:, LANES:]
        for k in range(n_half):
            bt_v[i * n_half + k] = bc_val[k * CHUNK:(k + 1) * CHUNK, :LANES].astype(F32).T.astype(BF16)

    project_bc(0)
    c_log = cum[:, :LANES]
    e_log = cum[:, LANES:]
    ct_v[...] = c_log.reshape(n_chunk, 16, LANES)
    et_v[...] = e_log.reshape(n_chunk, 16, LANES)
    tail = c_log[:, LANES - 1:LANES]
    parts_ef = split3(jnp.exp2(c_log))
    parts_eb = split3(jnp.exp2(tail - e_log))
    parts_wf = split3(jnp.exp2(tail - c_log) * dt_all)
    parts_wb = split3(jnp.exp2(e_log) * dt_all)
    project_bc(1)
    blank = jnp.zeros((16, LANES), F32)

    def row_tile(first, second, c):
        rows = slice(c * 16, (c + 1) * 16)
        tile = [p[rows].astype(F32) for p in first] + [blank] + [p[rows].astype(F32) for p in second] + [blank]
        return jnp.concatenate(tile, axis=0)

    def column_tile(first, second, c):
        return row_tile(first, second, c).T.astype(BF16)

    run = jnp.zeros((1, 32), F32)
    tails, starts, ends = [], [], []
    for c in range(n_chunk):
        rows = slice(c * 16, (c + 1) * 16)
        colb_v[c] = column_tile(parts_wf, parts_wb, c)
        cola_v[c] = row_tile(parts_ef, parts_eb, c)
        col = jnp.concatenate([c_log[rows], e_log[rows]], axis=0).T
        last = col[CHUNK - 1:CHUNK, :]
        tails.append(last)
        starts.append(run)
        run = run + last
        ends.append(run)
    logs = jnp.concatenate(tails + starts + [run - e for e in ends] + [run] * n_chunk, axis=0)
    tab = sum(dot(part, e_one) for part in split3(jnp.exp2(logs)))
    for i in range(3 * n_chunk + 1):
        tab_v[i] = tab[i:i + 1, :]
    dec_send[...] = tab[3 * n_chunk:, :]

    ld_wz.start()
    ld_wo.start()

    def to_partner(g):
        return pltpu.make_async_remote_copy(src_ref=s1_send[g], dst_ref=s1_recv[g], send_sem=s1_ss.at[g], recv_sem=s1_rs.at[g],
                                            device_id={'sp': partner}, device_id_type=MESH)

    def to_chip(g, t):
        return pltpu.make_async_remote_copy(src_ref=s2_send[g], dst_ref=s2_recv[g], send_sem=s2_ss.at[g, t], recv_sem=s2_rs.at[g],
                                            device_id={'sp': 2 - 2 * (sp // 2) + t}, device_id_type=MESH)

    def to_peer(g, k):
        return pltpu.make_async_remote_copy(src_ref=g_v[g].at[peer_base + k], dst_ref=g_recv[g].at[k], send_sem=g_ss.at[g, k],
                                            recv_sem=g_rs.at[g, k], device_id={'tp': other_tp}, device_id_type=MESH)

    def gather(i):
        owner = lax.rem(sp + 2, n_sp) if i == 2 else sp
        block = wo_peer.at[pl.ds(owner * wrows, wrows)]
        target = lax.rem(sp + 2, n_sp) if i == 1 else partner
        return pltpu.make_async_remote_copy(src_ref=block, dst_ref=block, send_sem=wf_ss.at[i], recv_sem=wf_rs.at[i],
                                            device_id={'sp': target}, device_id_type=MESH)

    dec_copy = pltpu.make_async_remote_copy(src_ref=dec_send, dst_ref=dec_recv, send_sem=dec_ss, recv_sem=dec_rs,
                                            device_id={'sp': partner}, device_id_type=MESH)
    dec_copy.start()

    def project_u(g):
        cols = slice(edge[g], edge[g + 1])
        for i in range(2):
            rows = slice(i * half, (i + 1) * half)
            u_v[rows, cols] = dot(x_v[rows, :], wx_v[:, cols]).astype(BF16)

    def states(g):
        for lo in range(edge[g], edge[g + 1], LANES):
            cols = slice(lo, lo + LANES)
            pick = pick_v[:, 2 * lo:2 * lo + 2 * LANES]
            acc = jnp.zeros((LANES, LANES), F32)
            for c in range(n_chunk):
                u_c = u_v[c * CHUNK:(c + 1) * CHUNK, cols].astype(F32)
                w_c = dot(colb_v[c], pick)
                u_w = jnp.concatenate([u_c * w_c[:, :LANES], u_c * w_c[:, LANES:]], axis=1).astype(BF16)
                st = dot(bt_v[c], u_w)
                pf_v[c, :, cols] = acc
                acc = tab_v[c][:, cols] * acc + st[:, :LANES]
                pb_v[c, :, cols] = st[:, LANES:]
            pf_v[n_chunk, :, cols] = acc
            acc = jnp.zeros((LANES, LANES), F32)
            for c in reversed(range(n_chunk)):
                st = pb_v[c, :, cols]
                pb_v[c, :, cols] = acc
                acc = tab_v[c][:, cols] * acc + st
            pb_v[n_chunk, :, cols] = acc
            s1_send[g][:, lo - edge[g]:lo - edge[g] + LANES] = jnp.where(core == 0, pf_v[n_chunk, :, cols], acc).astype(BF16)
        to_partner(g).start()

    sends_far = (sp == 1) | (sp == 2)

    def pass_on(g):
        to_partner(g).wait_recv()

        @pl.when(sends_far)
        def _():
            cols = slice(edge[g], edge[g + 1])
            own = jnp.where(core == 1, pf_v[n_chunk, :, cols], pb_v[n_chunk, :, cols])
            s2_send[g][...] = (own + tab_v[3 * n_chunk][:, cols] * s1_recv[g][...].astype(F32)).astype(BF16)
            to_chip(g, 0).start()
            to_chip(g, 1).start()

    def incoming(g):
        to_chip(g, 0).wait_recv()
        cols = slice(edge[g], edge[g + 1])
        near = s1_recv[g][...].astype(F32)
        far = s2_recv[g][...].astype(F32)
        both = near + dec_recv[0:1, cols] * far
        hf_v[:, cols] = jnp.where(sp == 0, 0.0, jnp.where(sp == 1, near, jnp.where(sp == 2, far, both)))
        hb_v[:, cols] = jnp.where(sp == 3, 0.0, jnp.where(sp == 2, near, jnp.where(sp == 1, far, both)))

    lane = lax.broadcasted_iota(jnp.int32, (CHUNK, LANES), 1)
    low_lane = lane < head_dim
    above = sq_r < sq_c
    below = sq_r > sq_c

    def project_z(g, base):
        cols = slice(edge[g], edge[g + 1])
        rows = pl.ds(pl.multiple_of(base * CHUNK, CHUNK), half)
        z_v[rows, cols] = dot(x_v[rows, :], wz_v[:, cols]).astype(BF16)

    def intra(g, c):
        rows = pl.ds(pl.multiple_of(c * CHUNK, CHUNK), CHUNK)
        gram = gram_v[c]
        for lo in range(edge[g], edge[g + 1], LANES):
            lanes = slice(lo, lo + LANES)
            h0 = lo // head_dim
            u_pair = u_v[rows, lanes]
            weights = []
            for h in (h0, h0 + 1):
                incl = ct_v[c, h:h + 1, :]
                excl = et_v[c, h:h + 1, :]
                gap = jnp.where(above, incl, excl).T - jnp.where(below, incl, excl)
                weights.append((gram * jnp.exp2(jnp.minimum(gap, -gap)) * dt_v[c, h:h + 1, :]).astype(BF16))
            zero = jnp.zeros_like(u_pair)
            u_diag = jnp.concatenate([jnp.where(low_lane, u_pair, zero), jnp.where(low_lane, zero, u_pair)], axis=0)
            skip = jnp.where(low_lane[:1], 2.0 * dskip_s[h0], 2.0 * dskip_s[h0 + 1])
            y_v[rows, lanes] = dot(jnp.concatenate(weights, axis=1), u_diag) + skip * u_pair.astype(F32)

    def finish(g, c):
        rows = pl.ds(pl.multiple_of(c * CHUNK, CHUNK), CHUNK)
        c_mat = c_v[rows, :]
        for lo in range(edge[g], edge[g + 1], LANES):
            cols = slice(lo, lo + LANES)
            in_f = pf_v[c, :, cols] + tab_v[n_chunk + c][:, cols] * hf_v[:, cols]
            in_b = pb_v[c, :, cols] + tab_v[2 * n_chunk + c][:, cols] * hb_v[:, cols]
            w_c = dot(colx_v[c], pick_v[:, 2 * lo:2 * lo + 2 * LANES])
            y_in = w_c * dot(c_mat, jnp.concatenate([in_f, in_b], axis=1).astype(BF16))
            y = y_v[rows, cols] + y_in[:, :LANES] + y_in[:, LANES:]
            hz = 0.5 * z_v[rows, cols].astype(F32)
            g_v[g][c, :, lo - edge[g]:lo - edge[g] + LANES] = (y * (hz + hz * jnp.tanh(hz))).astype(BF16)

    def gram_part(base):
        for k in range(n_half):
            c = base + k
            colx_v[c] = cola_v[c].T.astype(BF16)
            gram_v[c] = dot(c_v[pl.ds(pl.multiple_of(c * CHUNK, CHUNK), CHUNK), :], bt_v[c]) * diag2

    def send_finished(g):
        incoming(g)
        for k in range(n_half):
            finish(g, peer_base + k)
            to_peer(g, k).start()

    states(0)
    ld_wx.wait()
    project_u(1)
    pass_on(0)
    gram_part(peer_base)
    states(1)
    ld_wz.wait()
    project_z(0, peer_base)
    for k in range(n_half):
        intra(0, peer_base + k)
    pass_on(1)
    dec_copy.wait_recv()
    send_finished(0)
    project_z(1, peer_base)
    for k in range(n_half):
        intra(1, peer_base + k)
    project_u(2)
    states(2)
    pass_on(2)
    send_finished(1)
    wy.wait_recv()
    gather(0).start()
    gather(1).start()
    project_z(2, peer_base)
    for k in range(n_half):
        intra(2, peer_base + k)
    send_finished(2)

    gram_part(my_base)
    for g in range(n_grp):
        project_z(g, my_base)
        for k in range(n_half):
            intra(g, my_base + k)
        for k in range(n_half):
            finish(g, my_base + k)
    gather(1).wait_recv()
    gather(2).start()
    ld_wo.wait()
    my_tokens = pl.ds(pl.multiple_of(my_base * CHUNK, CHUNK), half)
    acc_v[...] = x_v[my_tokens, :].astype(F32)
    for g in range(n_grp):
        mine = g_v[g][pl.ds(my_base, n_half)].reshape(half, edge[g + 1] - edge[g])
        acc_v[...] += dot(mine, wo_own[edge[g]:edge[g + 1], :])
    gather(0).wait_recv()
    gather(2).wait_recv()
    for g in range(n_grp):
        w_g = wo_peer[edge[g]:edge[g + 1], :]
        for k in range(n_half):
            to_peer(g, k).wait_recv()
            rows = slice(k * CHUNK, (k + 1) * CHUNK)
            val = acc_v[rows, :] + dot(g_recv[g][k], w_g)
            if g < n_grp - 1:
                acc_v[rows, :] = val
            else:
                out_ref[rows, :] = val.astype(BF16)

    wy.wait_send()
    dec_copy.wait_send()
    for i in range(3):
        gather(i).wait_send()
    for g in range(n_grp):
        to_partner(g).wait_send()

        @pl.when(sends_far)
        def _():
            to_chip(g, 0).wait_send()
            to_chip(g, 1).wait_send()
        for k in range(n_half):
            to_peer(g, k).wait_send()


def solution(mesh):
    n_sp = mesh.shape['sp']

    def device_fn(x_blk, w_z, w_x, w_bc, w_dt, a_neg, dt_bias, d_skip, w_out):
        tokens, d_model = x_blk.shape
        n_head = a_neg.shape[0]
        inner = w_x.shape[1]
        half = tokens // 2
        n_chunk = tokens // CHUNK
        n_half = n_chunk // 2
        n_grp = len(GROUPS)
        wide = [LANES * p for p in GROUPS]
        vmem = pltpu.VMEM
        dma = pltpu.SemaphoreType.DMA
        state = [vmem((LANES, w), BF16) for w in wide]
        hbm = pl.BlockSpec(memory_space=pltpu.HBM)
        smem = pl.BlockSpec(memory_space=pltpu.SMEM)

        def body(*refs):
            kernel((tokens, n_head, n_sp), *refs)

        return pl.pallas_call(
            body,
            out_shape=pltpu.VMEM((half, d_model), BF16),
            in_specs=[hbm] * 6 + [smem] * 3,
            out_specs=pl.BlockSpec(memory_space=pltpu.VMEM),
            scratch_shapes=[
                vmem((tokens, d_model), BF16), vmem((d_model, inner), BF16), vmem((d_model, inner), BF16), vmem((d_model, 2 * LANES), BF16),
                vmem(w_bc.shape, BF16), vmem(w_dt.shape[::-1], BF16), vmem((inner, d_model), BF16), vmem((inner, d_model), BF16),
                vmem((tokens, LANES), BF16), vmem((n_chunk, LANES, CHUNK), BF16), vmem((LANES, d_model), F32),
                vmem((n_chunk, 16, LANES), F32), vmem((n_chunk, 16, LANES), F32), vmem((n_chunk, 16, LANES), F32),
                vmem((n_chunk, LANES, CHUNK), F32), vmem((n_chunk, CHUNK, LANES), BF16), vmem((n_chunk, CHUNK, LANES), BF16),
                vmem((LANES, 2 * inner), BF16), vmem((3 * n_chunk + 1, 1, inner), F32),
                vmem((n_chunk, CHUNK, CHUNK), F32),
                vmem((tokens, inner), BF16), vmem((tokens, inner), BF16), vmem((tokens, inner), F32),
                vmem((n_chunk + 1, LANES, inner), F32), vmem((n_chunk + 1, LANES, inner), F32),
                vmem((LANES, inner), F32), vmem((LANES, inner), F32), vmem((8, inner), F32), vmem((8, inner), F32),
                vmem((half, d_model), F32), state, state, state, state,
                [vmem((n_chunk, CHUNK, w), BF16) for w in wide], [vmem((n_half, CHUNK, w), BF16) for w in wide],
                dma((8,)), dma((n_grp,)), dma((n_grp,)), dma, dma, dma((n_grp, 2)), dma((n_grp,)),
                dma, dma, dma((3,)), dma((3,)), dma((n_grp, n_half)), dma((n_grp, n_half)),
            ],
            compiler_params=pltpu.CompilerParams(collective_id=0, has_side_effects=True, vmem_limit_bytes=56 * 2 ** 20),
            cost_estimate=pl.CostEstimate(flops=8 * 10 ** 9, bytes_accessed=8 * 10 ** 6, transcendentals=4 * 10 ** 6),
            name='mamba_layer',
        )(x_blk, w_z, w_x, w_bc, w_dt.T, w_out, a_neg, dt_bias, d_skip)

    in_specs = (P(('dp', 'sp'), None), P(None, 'tp'), P(None, 'tp'), P(None, None), P(None, 'tp'), P('tp'), P('tp'), P('tp'), P('tp', None))
    out_specs = P(('dp', 'sp', 'tp'), None)
    return jax.shard_map(device_fn, mesh=mesh, in_specs=in_specs, out_specs=out_specs, check_vma=False)
```
